32 devices in a mesh: head: 4 (over x, core), ctx: 8 (over z, y).
Axes of the slice: x: 2, y: 2, z: 4, core: 2. Of those that a mesh axis runs over, the one named last changes fastest.
Arguments:
- token_ids: int32 [2, 16], replicated, may hold values from 0 to 64127
- suffix_lengths: int32 [16], replicated, may hold values from 0 to 128, as said below
- embedding: bfloat16 [64128, 16384], P('ctx', 'head'), may hold values from -36 to 36
- attn_gain: float32 [16384], P('head'), may hold values from 0.25 to 1.75
- qkv_weight: bfloat16 [16384, 8, 1280], P('head', None, 'ctx'), may hold values from -0.046875 to 0.046875
- out_weight: bfloat16 [8192, 16384], P('head', 'ctx'), may hold values from -0.0625 to 0.0625
- prefix_keys: bfloat16 [8, 32768, 128], P('head', 'ctx'), may hold values from -32 to 32
- prefix_values: bfloat16 [8, 32768, 128], P('head', 'ctx'), may hold values from -8 to 8
- suffix_keys: bfloat16 [16, 128, 8, 128], P('ctx', None, 'head'), may hold values from -32 to 32
- suffix_values: bfloat16 [16, 128, 8, 128], P('ctx', None, 'head'), may hold values from -12 to 12
Outputs:
- attn_out: bfloat16 [16, 2, 16384], P('head', None, 'ctx')
The draws below stay inside these ranges and needn't reach their ends.
Inputs may be any that keep to these rules, and one draw needn't show every extreme that they name: Sequence b's suffix cache holds its tokens in slots 0 .. suffix_lengths[b] - 1; some sequence fills all 128 slots.
All inputs are finite; a program needn't handle non-finite values.
Results may differ from the reference program's by a relative error of at most 0.02.
Values may be sent and summed in bfloat16 or wider, within the bound.
No kernel may reach another device: no remote copies, remote signals or barrier semaphores. Data moves between devices by JAX's collectives and lax.ppermute only.
A program may use at most 128 MiB of HBM per device.

```python
import math
import jax
import jax.numpy as jnp
import numpy as np
from jax import lax

D = 16384
KVH = 8
HD = 128
GQ = 8
VOCAB = 64128
SUF = 128
STEPS = 2
CTX_DEV = 4096
B = 16
PREFIX = 32768
QW = 8192
UNITED = 1280
N_CTX = 8


def full_sequence(key):
    return jax.random.randint(jax.random.fold_in(key, 12), (), 0, B)


def draw_suffix_lengths(key, part):
    key_lengths = jax.random.fold_in(key, 11)
    lengths = jax.random.randint(key_lengths, (B,), 0, SUF + 1)
    return jnp.where(jnp.arange(B) == full_sequence(key), SUF, lengths).astype(jnp.int32)


def draw_embedding(key, part):
    key_rows = jax.random.fold_in(key, 21)
    key_cols = jax.random.fold_in(key, 22)
    key_base = jax.random.fold_in(key, 23)
    row_scale = jnp.exp(jax.random.uniform(key_rows, (VOCAB, 1), minval=math.log(0.3), maxval=math.log(3.0)))
    col_scale = jnp.exp(jax.random.uniform(key_cols, (1, D), minval=math.log(0.3), maxval=math.log(1.0)))
    place = jnp.arange(D).astype(jnp.float32)[None, :] / max(D - 1, 1)
    ramp = jnp.exp(math.log(3.0) * place)
    base_draw = jnp.clip(jax.random.normal(key_base, (VOCAB, D)), -4.0, 4.0)
    return (base_draw * row_scale * col_scale * ramp).astype(jnp.bfloat16)


def draw_qkv_weight(key, part):
    base_draw = jnp.clip(jax.random.normal(jax.random.fold_in(key, 61), (D, KVH, UNITED)), -4.0, 4.0) * D ** (-0.5)
    return base_draw.astype(jnp.bfloat16)


def draw_prefix_keys(key, part):
    key_base = jax.random.fold_in(key, 31)
    blocks = PREFIX // CTX_DEV
    base_draw = jnp.clip(5.0 * jax.random.normal(key_base, (KVH, blocks, CTX_DEV, HD)), -20.0, 20.0)
    return base_draw.reshape(KVH, PREFIX, HD).astype(jnp.bfloat16)


def draw_suffix_keys(key, part):
    key_base = jax.random.fold_in(key, 71)
    base_draw = jnp.clip(5.0 * jax.random.normal(key_base, (B, SUF, KVH, HD)), -20.0, 20.0)
    return base_draw.astype(jnp.bfloat16)


def draw_prefix_values(key, part):
    key_base = jax.random.fold_in(key, 41)
    key_offset = jax.random.fold_in(key, 42)
    blocks = PREFIX // CTX_DEV
    base_draw = jnp.clip(jax.random.normal(key_base, (KVH, blocks, CTX_DEV, HD)), -4.0, 4.0)
    offsets = jnp.clip(2.0 * jax.random.normal(key_offset, (KVH, blocks, 1, HD)), -4.0, 4.0)
    return (base_draw + offsets).reshape(KVH, PREFIX, HD).astype(jnp.bfloat16)


def touch_ends(drawn, own_key, least, high):
    longest = drawn.shape.index(max(drawn.shape))
    spots = []
    for shift in (0, 1):
        where = [jax.random.randint(jax.random.fold_in(own_key, axis), (), 0, length) for axis, length in enumerate(drawn.shape)]
        where[longest] = (where[longest] + shift) % drawn.shape[longest]
        spots.append(tuple(where))
    return drawn.at[spots[0]].set(least).at[spots[1]].set(high)


def levels(rng, shape, pieces, least, largest):
    def one(position, parts):
        heights = jax.random.uniform(jax.random.fold_in(jax.random.fold_in(rng, 6), position), (parts,), jnp.float32, least / len(pieces), largest / len(pieces))
        return jnp.repeat(jnp.exp(heights), shape[position] // parts).reshape((-1,) + (1,) * (len(shape) - position - 1))

    loudness = one(*pieces[0])
    for cut in pieces[1:]:
        loudness = loudness * one(*cut)
    return loudness


def rank_bounds(amount, lean):
    weights = [(1 << 20) // math.isqrt(rank ** lean) + 1 for rank in range(1, amount + 1)]
    scale = 1 + sum(weights) // (1 << 30)
    return np.cumsum(np.array([max(1, weight // scale) for weight in weights]))


def ranked(stream_key, extent, amount, slope):
    grid = rank_bounds(amount, slope)
    ticket = jax.random.randint(jax.random.fold_in(stream_key, 1), extent, 0, int(grid[amount - 1]))
    grade = jnp.searchsorted(jnp.asarray(grid, jnp.int32), ticket, side="right")
    return jax.random.permutation(jax.random.fold_in(stream_key, 2), amount)[grade].astype(jnp.int32)


def bell_draw(own_key, dims, scale, bound, pieces=(), kind=jnp.bfloat16):
    level = levels(own_key, dims, pieces, -0.22, 0.18) if pieces else 1.0
    values = jax.random.normal(own_key, dims, jnp.float32) * scale * level
    return jnp.minimum(jnp.maximum(values, -bound), bound).astype(kind)


def setup_inputs(seed: int = 0) -> dict:
    key_list = jax.random.split(jax.random.key(seed), 11)
    return {
        "token_ids": touch_ends(ranked(key_list[0], (STEPS, B), VOCAB, 2), jax.random.fold_in(key_list[0], 3), 0, VOCAB - 1).astype(jnp.int32),
        "suffix_lengths": draw_suffix_lengths(jax.random.fold_in(key_list[10], 71), 0),
        "embedding": draw_embedding(jax.random.fold_in(key_list[10], 71), 0),
        "attn_gain": jnp.clip(1.0 + 0.15 * jax.random.normal(key_list[3], (D,), jnp.float32), 0.25, 1.75),
        "qkv_weight": draw_qkv_weight(jax.random.fold_in(key_list[10], 71), 0),
        "out_weight": bell_draw(key_list[5], (QW, D), QW ** -0.5, 0.0625, ((0, 4), (1, 8))),
        "prefix_keys": draw_prefix_keys(jax.random.fold_in(key_list[10], 71), 0),
        "prefix_values": draw_prefix_values(jax.random.fold_in(key_list[10], 71), 0),
        "suffix_keys": draw_suffix_keys(jax.random.fold_in(key_list[10], 71), 0),
        "suffix_values": bell_draw(key_list[9], (B, SUF, KVH, HD), 2.0, 12.0, ((0, 8), (2, 4))),
    }


EPSILON = 1e-05
ROTARY_THETA = 500000.0
MASKED = -1e+30

def rotary(vectors, positions):
    half_width = vectors.shape[-1] // 2
    frequency = ROTARY_THETA ** (-2.0 * jnp.arange(half_width).astype(jnp.float32) / vectors.shape[-1])
    angles = positions[..., None] * frequency
    cosine = jnp.cos(angles)
    sine_values = jnp.sin(angles)
    front_half = vectors[..., :half_width]
    back_half = vectors[..., half_width:]
    return jnp.concatenate([front_half * cosine - back_half * sine_values, back_half * cosine + front_half * sine_values], axis=-1)

def rounded(values):
    return lax.optimization_barrier(values.astype(jnp.bfloat16)).astype(jnp.float32)

def combine(earlier, later):
    highest = jnp.maximum(earlier[0], later[0])
    first_scale = jnp.exp(earlier[0] - highest)
    second_scale = jnp.exp(later[0] - highest)
    return (highest, earlier[1] * first_scale + later[1] * second_scale, earlier[2] * first_scale[..., None] + later[2] * second_scale[..., None])

def weigh_scores(scores):
    maxima = lax.optimization_barrier(jnp.max(scores, axis=-1))
    weights = rounded(jnp.exp(scores - maxima[..., None]))
    return (maxima, weights, lax.optimization_barrier(jnp.sum(weights, axis=-1)))

def reference(token_ids, suffix_lengths, embedding, attn_gain, qkv_weight, out_weight, prefix_keys, prefix_values, suffix_keys, suffix_values):
    embedded = embedding[token_ids]
    features = embedded.astype(jnp.float32)
    mean_sq = lax.optimization_barrier(jnp.mean(features * features, axis=-1))
    normed = (features * lax.rsqrt(mean_sq + EPSILON)[..., None] * attn_gain).astype(jnp.bfloat16)
    qkv_rows = jnp.dot(normed.reshape(STEPS * B, D), qkv_weight.reshape(D, KVH * UNITED), preferred_element_type=jnp.float32)
    qkv_rows = qkv_rows.astype(jnp.bfloat16).reshape(STEPS, B, KVH, UNITED)
    query_width = GQ * HD
    queries = qkv_rows[..., :query_width].reshape(STEPS, B, KVH, GQ, HD)
    new_keys = qkv_rows[..., query_width:query_width + HD]
    new_values = qkv_rows[..., query_width + HD:]
    positions = (PREFIX + suffix_lengths[None, :] + jnp.arange(STEPS, dtype=jnp.int32)[:, None]).astype(jnp.float32)
    queries_rot = (rotary(queries.astype(jnp.float32), positions[:, :, None, None]) * HD ** (-0.5)).astype(jnp.bfloat16)
    keys_rot = rotary(new_keys.astype(jnp.float32), positions[:, :, None]).astype(jnp.bfloat16)
    live_slots = jnp.arange(SUF, dtype=jnp.int32)[None, :] < suffix_lengths[:, None]
    visible = jnp.arange(STEPS, dtype=jnp.int32)[None, :] <= jnp.arange(STEPS, dtype=jnp.int32)[:, None]
    row_count = STEPS * B * GQ

    def one_head(head_index):
        head_queries = lax.dynamic_index_in_dim(queries_rot, head_index, 2, keepdims=False).astype(jnp.float32)
        flat_queries = head_queries.reshape(row_count, HD)
        cache_keys = lax.dynamic_index_in_dim(prefix_keys, head_index, 0, keepdims=False)
        cache_values = lax.dynamic_index_in_dim(prefix_values, head_index, 0, keepdims=False)

        def block_step(running, block_index):
            block_start = (block_index * CTX_DEV).astype(jnp.int32)
            keys_block = lax.dynamic_slice_in_dim(cache_keys, block_start, CTX_DEV, 0).astype(jnp.float32)
            values_block = lax.dynamic_slice_in_dim(cache_values, block_start, CTX_DEV, 0).astype(jnp.float32)
            scores = jnp.dot(flat_queries, keys_block.T, precision=lax.Precision.HIGHEST)
            maxima, weights, totals = weigh_scores(scores)
            sums = jnp.dot(weights, values_block, precision=lax.Precision.HIGHEST)
            return (combine(running, (maxima, totals, sums)), None)
        initial = (jnp.full((row_count,), MASKED, dtype=jnp.float32), jnp.zeros((row_count,), jnp.float32), jnp.zeros((row_count, HD), jnp.float32))
        running, unused = lax.scan(block_step, initial, jnp.arange(N_CTX, dtype=jnp.int32))
        slot_keys = lax.dynamic_index_in_dim(suffix_keys, head_index, 2, keepdims=False).astype(jnp.float32)
        slot_values = lax.dynamic_index_in_dim(suffix_values, head_index, 2, keepdims=False).astype(jnp.float32)
        fresh_keys = lax.dynamic_index_in_dim(keys_rot, head_index, 2, keepdims=False).astype(jnp.float32)
        fresh_values = lax.dynamic_index_in_dim(new_values, head_index, 2, keepdims=False).astype(jnp.float32)
        slot_scores = jnp.einsum('tbjd,bsd->tbjs', head_queries, slot_keys, precision=lax.Precision.HIGHEST)
        slot_scores = jnp.where(live_slots[None, :, None, :], slot_scores, MASKED)
        fresh_scores = jnp.einsum('tbjd,ubd->tbju', head_queries, fresh_keys, precision=lax.Precision.HIGHEST)
        fresh_scores = jnp.where(visible[:, None, None, :], fresh_scores, MASKED)
        maxima, weights, totals = weigh_scores(jnp.concatenate([slot_scores, fresh_scores], axis=-1))
        numerators = jnp.einsum('tbjs,bsd->tbjd', weights[..., :SUF], slot_values, precision=lax.Precision.HIGHEST)
        numerators = numerators + jnp.einsum('tbju,ubd->tbjd', weights[..., SUF:], fresh_values, precision=lax.Precision.HIGHEST)
        far_part = (running[0].reshape(STEPS, B, GQ), running[1].reshape(STEPS, B, GQ), running[2].reshape(STEPS, B, GQ, HD))
        merged = combine(far_part, (maxima, totals, numerators))
        return (merged[2] / merged[1][..., None]).astype(jnp.bfloat16)
    per_head = lax.map(one_head, jnp.arange(KVH, dtype=jnp.int32))
    attention = jnp.transpose(per_head, (1, 2, 0, 3, 4)).reshape(STEPS * B, KVH * GQ * HD)
    projected = jnp.dot(attention, out_weight, preferred_element_type=jnp.float32).reshape(STEPS, B, D)
    return jnp.transpose(projected, (1, 0, 2)).astype(jnp.bfloat16)
```

```python
import jax
import jax.numpy as jnp
from jax import lax
from jax.sharding import PartitionSpec as P

EPSILON = 1e-05
ROTARY_THETA = 500000.0
MASKED = -1e30
BF16 = jnp.bfloat16
F32 = jnp.float32


def exchange(blocks, axis):
    return lax.all_to_all(blocks, axis, 0, 0)


def gather_all(block, axis):
    count = lax.axis_size(axis)
    return exchange(jnp.broadcast_to(block[None], (count,) + block.shape), axis)


def scatter_direct(blocks, axis):
    count = lax.axis_size(axis)
    here = lax.axis_index(axis)
    received = [lax.dynamic_index_in_dim(blocks, here, 0, False)]
    for shift in range(1, count):
        target = lax.rem(here + shift, count)
        piece = lax.dynamic_index_in_dim(blocks, target, 0, False)
        pairs = [(i, (i + shift) % count) for i in range(count)]
        received.append(lax.ppermute(piece, axis, pairs))
    return received


def rotary_tables(positions, head_dim):
    half_width = head_dim // 2
    frequency = ROTARY_THETA ** (-2.0 * jnp.arange(half_width).astype(F32) / head_dim)
    angles = positions[..., None] * frequency
    return jnp.cos(angles), jnp.sin(angles)


def rotate(vectors, cosine, sine):
    half_width = vectors.shape[-1] // 2
    front = vectors[..., :half_width]
    back = vectors[..., half_width:]
    return jnp.concatenate([front * cosine - back * sine, back * cosine + front * sine], axis=-1)


def body(
    token_ids,
    suffix_lengths,
    embedding,
    attn_gain,
    qkv_weight,
    out_weight,
    prefix_keys,
    prefix_values,
    suffix_keys,
    suffix_values,
):
    steps, batch = token_ids.shape
    rows = steps * batch
    n_ctx = lax.axis_size("ctx")
    n_head = lax.axis_size("head")
    local_heads, _, head_dim = prefix_keys.shape
    width = embedding.shape[1]
    slots = suffix_keys.shape[1]
    owned = suffix_keys.shape[0]
    mine = lax.axis_index("ctx")
    tokens = token_ids.T.reshape(rows)
    offsets = tokens - mine * embedding.shape[0]
    inside = (offsets >= 0) & (offsets < embedding.shape[0])
    picked = jnp.take(embedding, jnp.clip(offsets, 0, embedding.shape[0] - 1), axis=0)
    picked = jnp.where(inside[:, None], picked, jnp.zeros((), BF16))
    arrived = exchange(picked.reshape(n_ctx, rows // n_ctx, width), "ctx")
    chunk = jnp.sum(arrived.astype(F32), axis=0).astype(BF16)
    features = gather_all(chunk, "ctx").reshape(rows, width).astype(F32)
    square_sum = jnp.sum(features * features, axis=-1)
    scaled = (features * attn_gain).astype(BF16)
    partial = jnp.einsum("rd,dgf->grf", scaled, qkv_weight, preferred_element_type=F32)
    partial = partial.reshape(n_head, local_heads, rows, -1)
    square_sum = jnp.broadcast_to(square_sum[None, None, :, None], (n_head, local_heads, rows, 1))
    pieces = scatter_direct(jnp.concatenate([partial, square_sum], axis=-1), "head")
    total = sum(pieces[1:], pieces[0])
    factor = lax.rsqrt(total[..., -1:] / (width * n_head) + EPSILON)
    columns = (total[..., :-1] * factor).astype(BF16)
    united = gather_all(columns, "ctx")
    united = jnp.transpose(united, (1, 2, 0, 3)).reshape(local_heads, batch, steps, -1)
    query_width = united.shape[-1] - 2 * head_dim
    group = query_width // head_dim
    queries = united[..., :query_width].reshape(local_heads, batch, steps, group, head_dim)
    step_index = jnp.arange(steps, dtype=jnp.int32)
    context = prefix_keys.shape[1] * n_ctx
    positions = (context + suffix_lengths[:, None] + step_index[None, :]).astype(F32)
    cosine, sine = rotary_tables(positions, head_dim)
    queries = (
        rotate(queries.astype(F32), cosine[:, :, None], sine[:, :, None]) * head_dim ** (-0.5)
    ).astype(BF16)
    flat = queries.reshape(local_heads, rows * group, head_dim)
    scores = jnp.einsum("gqd,gkd->gqk", flat, prefix_keys, preferred_element_type=F32)
    maxima = jnp.max(scores, axis=-1, keepdims=True)
    weights = jnp.exp(scores - maxima).astype(BF16)
    totals = jnp.sum(weights.astype(F32), axis=-1, keepdims=True)
    sums = jnp.einsum("gqk,gkd->gqd", weights, prefix_values, preferred_element_type=F32)
    packet = jnp.concatenate([sums, maxima, totals], axis=-1)
    packet = packet.reshape(local_heads, n_ctx, -1, head_dim + 2)
    packet = jnp.swapaxes(packet, 0, 1)
    parts = exchange(packet, "ctx")
    own = mine * owned
    near_queries = lax.dynamic_slice_in_dim(queries, own, owned, 1)
    near_keys = rotate(united[..., query_width : query_width + head_dim].astype(F32), cosine, sine)
    near_keys = lax.dynamic_slice_in_dim(near_keys.astype(BF16), own, owned, 1)
    near_values = lax.dynamic_slice_in_dim(united[..., query_width + head_dim :], own, owned, 1)
    lengths = lax.dynamic_slice_in_dim(suffix_lengths, own, owned, 0)
    slot_scores = jnp.einsum(
        "gbtjd,bsgd->gbtjs", near_queries, suffix_keys, preferred_element_type=F32
    )
    live = jnp.arange(slots, dtype=jnp.int32)[None, :] < lengths[:, None]
    slot_scores = jnp.where(live[None, :, None, None, :], slot_scores, MASKED)
    fresh = jnp.einsum("gbtjd,gbud->gbtju", near_queries, near_keys, preferred_element_type=F32)
    visible = step_index[None, :] <= step_index[:, None]
    fresh = jnp.where(visible[None, None, :, None, :], fresh, MASKED)
    near_scores = jnp.concatenate([slot_scores, fresh], axis=-1)
    near_max = jnp.max(near_scores, axis=-1, keepdims=True)
    near_weights = jnp.exp(near_scores - near_max).astype(BF16)
    near_total = jnp.sum(near_weights.astype(F32), axis=-1, keepdims=True)
    near_sum = jnp.einsum(
        "gbtjs,bsgd->gbtjd", near_weights[..., :slots], suffix_values, preferred_element_type=F32
    ) + jnp.einsum(
        "gbtju,gbud->gbtjd", near_weights[..., slots:], near_values, preferred_element_type=F32
    )
    near = jnp.concatenate([near_sum, near_max, near_total], axis=-1).reshape(parts.shape[1:])
    everything = jnp.concatenate([parts, near[None]], axis=0)
    highest = jnp.max(everything[..., head_dim : head_dim + 1], axis=0, keepdims=True)
    scale = jnp.exp(everything[..., head_dim : head_dim + 1] - highest)
    numerator = jnp.sum(everything[..., :head_dim] * scale, axis=0)
    denominator = jnp.sum(everything[..., head_dim + 1 :] * scale, axis=0)
    attention = (numerator / denominator).astype(BF16)
    attention = attention.reshape(local_heads, owned * steps, group * head_dim)
    attention = gather_all(attention, "ctx")
    attention = jnp.transpose(attention, (0, 2, 1, 3)).reshape(rows, -1)
    out = jnp.dot(attention, out_weight, preferred_element_type=F32).astype(BF16)
    out = out.reshape(n_head, rows // n_head, -1)
    pieces = scatter_direct(out, "head")
    result = sum([p.astype(F32) for p in pieces[1:]], pieces[0].astype(F32)).astype(BF16)
    return result.reshape(batch // n_head, steps, -1)


def solution(mesh):
    placed = (
        P(),
        P(),
        P("ctx", "head"),
        P("head"),
        P("head", None, "ctx"),
        P("head", "ctx"),
        P("head", "ctx", None),
        P("head", "ctx", None),
        P("ctx", None, "head", None),
        P("ctx", None, "head", None),
    )
    return jax.shard_map(
        body, mesh=mesh, in_specs=placed, out_specs=P("head", None, "ctx"), check_vma=False
    )
```

```python
import functools

import jax
import jax.numpy as jnp
from jax import lax
from jax.experimental import pallas as pl
from jax.experimental.pallas import tpu as pltpu
from jax.sharding import PartitionSpec as P

EPSILON = 1e-05
ROTARY_THETA = 500000.0
MASKED = -1e30
BF16 = jnp.bfloat16
F32 = jnp.float32
LANES = 128
MIB = 1 << 20
VMEM = pl.BlockSpec(memory_space=pltpu.VMEM)
SMEM = pl.BlockSpec(memory_space=pltpu.SMEM)
HBM = pl.BlockSpec(memory_space=pl.ANY)
NT = (((1,), (1,)), ((), ()))


def round_up(value, unit):
    return -(-value // unit) * unit


def params(limit):
    return pltpu.CompilerParams(vmem_limit_bytes=min(limit, 60 * MIB))


def cost(flops, moved, transcendentals=0):
    return pl.CostEstimate(flops=flops, bytes_accessed=moved, transcendentals=transcendentals)


def exchange(blocks, axis):
    return lax.all_to_all(blocks, axis, 0, 0)


def send_pieces(pieces, axis):
    count = lax.axis_size(axis)
    received = [pieces[0]]
    for shift in range(1, count):
        pairs = [(i, (i + shift) % count) for i in range(count)]
        received.append(lax.ppermute(pieces[shift], axis, pairs))
    return received


def lookup_kernel(tokens, table, out, blocks, rows_f32, sem):
    steps, batch = tokens.shape
    chunks, rows, width = out.shape
    local_rows = table.shape[0]
    base = lax.axis_index("ctx") * local_rows

    def place(row):
        offset = tokens[row % steps, row // steps] - base
        return offset, (offset >= 0) & (offset < local_rows)

    def copy(row, offset):
        start = pl.multiple_of((offset // 8) * 8, 8)
        return pltpu.make_async_copy(
            table.at[pl.ds(start, 8), :], blocks.at[row], sem.at[row]
        )

    for row in range(rows):
        offset, inside = place(row)

        @pl.when(inside)
        def _():
            copy(row, offset).start()

    rows_f32[...] = jnp.zeros_like(rows_f32)
    sublane = lax.broadcasted_iota(jnp.int32, (8, 1), 0)
    for row in range(rows):
        offset, inside = place(row)

        @pl.when(inside)
        def _():
            copy(row, offset).wait()
            picked = jnp.where(sublane == offset % 8, blocks[row].astype(F32), 0.0)
            rows_f32[row : row + 1, :] = jnp.sum(picked, axis=0, keepdims=True)

    for chunk in range(chunks):
        out[chunk] = rows_f32[:, chunk * width : (chunk + 1) * width].astype(BF16)


def lookup_rows(token_ids, embedding):
    steps, batch = token_ids.shape
    rows = steps * batch
    chunks = lax.axis_size("ctx")
    local_rows, width = embedding.shape
    if local_rows % 8 == 0:
        return pl.pallas_call(
            lookup_kernel,
            out_shape=jax.ShapeDtypeStruct((chunks, rows, width // chunks), BF16),
            in_specs=[SMEM, HBM],
            out_specs=VMEM,
            scratch_shapes=[
                pltpu.VMEM((rows, 8, width), BF16),
                pltpu.VMEM((rows, width), F32),
                pltpu.SemaphoreType.DMA((rows,)),
            ],
            compiler_params=params(6 * rows * width * 8),
            cost_estimate=cost(rows * width, rows * width * 16),
            name="lookup",
        )(token_ids, embedding)
    offsets = token_ids.T.reshape(rows) - lax.axis_index("ctx") * local_rows
    inside = (offsets >= 0) & (offsets < local_rows)
    picked = jnp.take(embedding, jnp.clip(offsets, 0, local_rows - 1), axis=0)
    picked = jnp.where(inside[:, None], picked, jnp.zeros((), BF16))
    return jnp.swapaxes(picked.reshape(rows, chunks, width // chunks), 0, 1)


def join_kernel(parts, out):
    total = parts[0].astype(F32)
    for source in range(1, parts.shape[0]):
        total = total + parts[source].astype(F32)
    joined = total.astype(BF16)
    for target in range(out.shape[0]):
        out[target] = joined


def join_copies(parts):
    return pl.pallas_call(
        join_kernel,
        out_shape=jax.ShapeDtypeStruct(parts.shape, BF16),
        in_specs=[VMEM],
        out_specs=VMEM,
        compiler_params=params(8 * MIB),
        name="join",
    )(parts)


def project_kernel(heads_here, x, gain, weight, *refs):
    count = weight.shape[0] // heads_here
    outs, (held, scaled, sem) = refs[:count], refs[count:]
    chunks, rows, chunk_width = x.shape
    columns = weight.shape[1]
    here = lax.axis_index("head")

    def copy(shift):
        first = lax.rem(here + shift, count) * heads_here
        return pltpu.make_async_copy(
            weight.at[pl.ds(first, heads_here)], held.at[shift], sem.at[shift]
        )

    for shift in range(count):
        copy(shift).start()
    squares = jnp.zeros((rows, 1), F32)
    for chunk in range(chunks):
        span = slice(chunk * chunk_width, (chunk + 1) * chunk_width)
        features = x[chunk].astype(F32)
        squares = squares + jnp.sum(features * features, axis=-1, keepdims=True)
        scaled[:, span] = (features * gain[:, span]).astype(BF16)
    used = heads_here * columns
    rest = outs[0].shape[1] - used
    for shift in range(count):
        copy(shift).wait()
        products = [
            lax.dot_general(scaled[...], held[shift, head], NT, preferred_element_type=F32)
            for head in range(heads_here)
        ]
        outs[shift][...] = jnp.concatenate(
            products + [jnp.broadcast_to(squares, (rows, rest))], axis=1
        )


def project(x, attn_gain, weight):
    count = lax.axis_size("head")
    chunks, rows, chunk_width = x.shape
    heads, columns, width = weight.shape
    heads_here = heads // count
    wide = round_up(heads_here * columns + 1, LANES)
    size = weight.size * 2
    return pl.pallas_call(
        functools.partial(project_kernel, heads_here),
        out_shape=[jax.ShapeDtypeStruct((rows, wide), F32)] * count,
        in_specs=[VMEM, VMEM, HBM],
        out_specs=[VMEM] * count,
        scratch_shapes=[
            pltpu.VMEM((count, heads_here, columns, width), BF16),
            pltpu.VMEM((rows, width), BF16),
            pltpu.SemaphoreType.DMA((count,)),
        ],
        compiler_params=params(size + 10 * MIB),
        cost_estimate=cost(2 * rows * weight.size, size),
        name="project",
    )(x, attn_gain.reshape(1, width), weight)


def norm_kernel(used, model_width, *refs):
    pieces, out = refs[:-1], refs[-1]
    total = pieces[0][...]
    for piece in pieces[1:]:
        total = total + piece[...]
    factor = lax.rsqrt(total[:, used : used + 1] * (1.0 / model_width) + EPSILON)
    united = (total * factor).astype(BF16)
    for target in range(out.shape[0]):
        out[target] = united


def norm_copies(pieces, used, model_width):
    rows, wide = pieces[0].shape
    return pl.pallas_call(
        functools.partial(norm_kernel, used, model_width),
        out_shape=jax.ShapeDtypeStruct((lax.axis_size("ctx"), rows, wide), BF16),
        in_specs=[VMEM] * len(pieces),
        out_specs=VMEM,
        compiler_params=params(8 * MIB),
        name="norm",
    )(*pieces)


def split3(value):
    first = value.astype(BF16).astype(F32)
    second = (value - first).astype(BF16).astype(F32)
    return first, second, value - first - second


def attend_kernel(columns, group, united, cosine, sine, keys, values, packet, ready, fresh, *scratch):
    key_buf, value_buf, query_buf, score_buf, key_sem, value_sem = scratch
    chunks, rows, _ = united.shape
    heads, context, head_dim = keys.shape
    per_dest = rows // chunks
    block = per_dest * group
    tile = min(512, context)
    tiles = context // tile

    def key_copy(head):
        return pltpu.make_async_copy(keys.at[head], key_buf.at[head], key_sem.at[head])

    def value_copy(head):
        return pltpu.make_async_copy(values.at[head], value_buf.at[head], value_sem.at[head])

    for head in range(heads):
        key_copy(head).start()
        value_copy(head).start()

    cos = cosine[...]
    sin = sine[...]

    def rotated(vectors):
        return vectors * cos + pltpu.roll(vectors, head_dim // 2, 1) * sin

    for head in range(heads):
        first = head * columns
        whole = jnp.concatenate(
            [united[chunk].astype(F32)[:, first : first + columns] for chunk in range(chunks)],
            axis=1,
        )
        for j in range(group):
            query = rotated(whole[:, j * head_dim : (j + 1) * head_dim]) * head_dim ** (-0.5)
            for dest in range(chunks):
                start = dest * block + j * per_dest
                query_buf[head, start : start + per_dest, :] = query[
                    dest * per_dest : (dest + 1) * per_dest
                ]
        new_key = whole[:, group * head_dim : (group + 1) * head_dim]
        fresh[head] = rotated(new_key).astype(BF16)
        fresh[heads + head] = whole[:, (group + 1) * head_dim :].astype(BF16)

    lane = lax.broadcasted_iota(jnp.int32, (chunks * block, LANES), 1)
    for head in range(heads):
        query = query_buf[head].astype(BF16)
        for dest in range(chunks):
            ready[dest, head] = query[dest * block : (dest + 1) * block]
        key_copy(head).wait()
        highest = None
        for step in range(tiles):
            span = slice(step * tile, (step + 1) * tile)
            scores = lax.dot_general(
                query, key_buf[head, span, :], NT, preferred_element_type=F32
            )
            score_buf[:, span] = scores
            for part in range(tile // LANES):
                piece = scores[:, part * LANES : (part + 1) * LANES]
                highest = piece if highest is None else jnp.maximum(highest, piece)
        maxima = jnp.max(highest, axis=-1, keepdims=True)
        value_copy(head).wait()
        sums = jnp.zeros((chunks * block, head_dim), F32)
        totals = jnp.zeros((chunks * block, LANES), F32)
        for step in range(tiles):
            span = slice(step * tile, (step + 1) * tile)
            weights = jnp.exp(score_buf[:, span] - maxima).astype(BF16)
            sums = sums + jnp.dot(weights, value_buf[head, span, :], preferred_element_type=F32)
            wide = weights.astype(F32)
            for part in range(tile // LANES):
                totals = totals + wide[:, part * LANES : (part + 1) * LANES]
        total = jnp.sum(totals, axis=-1, keepdims=True)
        table = jnp.zeros((chunks * block, LANES), F32)
        for index, piece in enumerate(split3(maxima) + split3(total)):
            table = jnp.where(lane == index, piece, table)
        rounded = sums.astype(BF16)
        for dest in range(chunks):
            packet[dest, head * block : (head + 1) * block] = rounded[
                dest * block : (dest + 1) * block
            ]
        turned = jnp.transpose(table)[:16]
        for dest in range(chunks):
            packet[dest, heads * block + head * 16 : heads * block + (head + 1) * 16, :block] = turned[
                :, dest * block : (dest + 1) * block
            ].astype(BF16)


def attend(united, columns, cosine, sine, keys, values):
    chunks, rows, _ = united.shape
    heads, context, head_dim = keys.shape
    group = columns * chunks // head_dim - 2
    block = rows // chunks * group
    size = keys.size * 2
    flat = chunks * block
    return pl.pallas_call(
        functools.partial(attend_kernel, columns, group),
        out_shape=[
            jax.ShapeDtypeStruct((chunks, heads * (block + 16), head_dim), BF16),
            jax.ShapeDtypeStruct((chunks, heads, block, head_dim), BF16),
            jax.ShapeDtypeStruct((2 * heads, rows, head_dim), BF16),
        ],
        in_specs=[VMEM, VMEM, VMEM, HBM, HBM],
        out_specs=[VMEM] * 3,
        scratch_shapes=[
            pltpu.VMEM(keys.shape, BF16),
            pltpu.VMEM(keys.shape, BF16),
            pltpu.VMEM((heads, flat, head_dim), F32),
            pltpu.VMEM((flat, context), F32),
            pltpu.SemaphoreType.DMA((heads,)),
            pltpu.SemaphoreType.DMA((heads,)),
        ],
        compiler_params=params(2 * size + flat * context * 4 + 16 * MIB),
        cost_estimate=cost(4 * heads * flat * context * head_dim, 2 * size, heads * flat * context),
        name="attend",
    )(united, cosine, sine, keys, values)


def near_kernel(owned, lengths, ready, fresh, keys, values, sums, maxima, totals):
    heads, rows, head_dim = fresh.shape
    heads //= 2
    _, _, block, _ = ready.shape
    slots_all = keys.shape[1]
    per_dest = rows // ready.shape[0]
    steps = per_dest // owned
    mine = lax.axis_index("ctx")

    def iota(shape, axis):
        return lax.broadcasted_iota(jnp.int32, shape, axis)

    query_place = iota((block, 1), 0) % per_dest
    sequence = query_place // steps
    step = query_place % steps
    slot = iota((1, slots_all), 1)
    fresh_row = iota((1, rows), 1)
    fresh_here = (fresh_row // steps == mine * owned + sequence) & (fresh_row % steps <= step)
    for head in range(heads):
        query = ready[mine, head]
        fresh_scores = lax.dot_general(query, fresh[head], NT, preferred_element_type=F32)
        fresh_scores = jnp.where(fresh_here, fresh_scores, MASKED)
        scores = []
        highest = jnp.max(fresh_scores, axis=-1, keepdims=True)
        for s in range(owned):
            found = lax.dot_general(query, keys[s], NT, preferred_element_type=F32)
            live = (sequence == s) & (slot % heads == head)
            live = live & (slot // heads < lengths[mine * owned + s])
            found = jnp.where(live, found, MASKED)
            scores.append(found)
            highest = jnp.maximum(highest, jnp.max(found, axis=-1, keepdims=True))
        weights = jnp.exp(fresh_scores - highest).astype(BF16)
        total = jnp.sum(weights.astype(F32), axis=-1, keepdims=True)
        result = jnp.dot(weights, fresh[heads + head], preferred_element_type=F32)
        for s in range(owned):
            weights = jnp.exp(scores[s] - highest).astype(BF16)
            total = total + jnp.sum(weights.astype(F32), axis=-1, keepdims=True)
            result = result + jnp.dot(weights, values[s], preferred_element_type=F32)
        span = slice(head * block, (head + 1) * block)
        sums[span, :] = result
        maxima[span, :] = jnp.broadcast_to(highest, (block, head_dim))
        totals[span, :] = jnp.broadcast_to(total, (block, head_dim))


def near(lengths, ready, fresh, keys, values):
    owned, slots, heads, head_dim = keys.shape
    block = ready.shape[2]
    shape = jax.ShapeDtypeStruct((heads * block, head_dim), F32)
    return pl.pallas_call(
        functools.partial(near_kernel, owned),
        out_shape=[shape] * 3,
        in_specs=[SMEM, VMEM, VMEM, VMEM, VMEM],
        out_specs=[VMEM] * 3,
        compiler_params=params(8 * MIB),
        cost_estimate=cost(4 * heads * block * owned * slots * heads * head_dim, keys.size * 4),
        name="near",
    )(
        lengths,
        ready,
        fresh,
        keys.reshape(owned, slots * heads, head_dim),
        values.reshape(owned, slots * heads, head_dim),
    )


def merge_kernel(group, parts, near_sums, near_maxima, near_totals, out, places, stats):
    chunks = parts.shape[0]
    per_dest = out.shape[1]
    block = per_dest * group
    queries, head_dim = near_sums.shape
    heads = queries // block
    highest = near_maxima[...][:, :1]
    maxima, totals = [], []
    for source in range(chunks):
        for head in range(heads):
            low = queries + head * 16
            found = parts[source, low : low + 16, :].astype(F32)[:8]
            row = (source * heads + head) * 8
            stats[row : row + 8, :] = found
    turned = jnp.transpose(stats[...])[:block]
    for source in range(chunks):
        m, t = [], []
        for head in range(heads):
            column = (source * heads + head) * 8
            get = lambda k: turned[:, column + k : column + k + 1]
            m.append(get(0) + get(1) + get(2))
            t.append(get(3) + get(4) + get(5))
        maxima.append(jnp.concatenate(m, axis=0))
        totals.append(jnp.concatenate(t, axis=0))
        highest = jnp.maximum(highest, maxima[-1])
    scale = jnp.exp(near_maxima[...][:, :1] - highest)
    numerator = near_sums[...] * scale
    denominator = near_totals[...][:, :1] * scale
    for source in range(chunks):
        scale = jnp.exp(maxima[source] - highest)
        numerator = numerator + parts[source, :queries, :].astype(F32) * scale
        denominator = denominator + totals[source] * scale
    attention = numerator / denominator
    for index in range(heads * group):
        places[:, index * head_dim : (index + 1) * head_dim] = attention[
            index * per_dest : (index + 1) * per_dest
        ]
    rounded = places[...].astype(BF16)
    for target in range(chunks):
        out[target] = rounded


def merge_copies(parts, sums, maxima, totals, group, per_dest):
    chunks = parts.shape[0]
    queries, head_dim = sums.shape
    heads = queries // (per_dest * group)
    width = heads * group * head_dim
    return pl.pallas_call(
        functools.partial(merge_kernel, group),
        out_shape=jax.ShapeDtypeStruct((chunks, per_dest, width), BF16),
        in_specs=[VMEM] * 4,
        out_specs=VMEM,
        scratch_shapes=[
            pltpu.VMEM((per_dest, width), F32),
            pltpu.VMEM((chunks * heads * 8, head_dim), F32),
        ],
        compiler_params=params(12 * MIB),
        name="merge",
    )(parts, sums, maxima, totals)


def output_kernel(x, weight, *refs):
    chunks, per_dest, depth = x.shape
    held, rows_f32, total, sem = refs[-4:]
    outs = refs[:-4]
    count = len(outs)
    pieces = held.shape[0]
    step = depth // pieces

    def copy(piece):
        return pltpu.make_async_copy(
            weight.at[pl.ds(piece * step, step), :], held.at[piece], sem.at[piece]
        )

    for piece in range(pieces):
        copy(piece).start()
    for chunk in range(chunks):
        rows_f32[chunk * per_dest : (chunk + 1) * per_dest, :] = x[chunk].astype(F32)
    rows = rows_f32[...].astype(BF16)
    for piece in range(pieces):
        copy(piece).wait()
        product = jnp.dot(
            rows[:, piece * step : (piece + 1) * step], held[piece], preferred_element_type=F32
        )
        if piece == 0:
            total[...] = product
        else:
            total[...] += product
    here = lax.axis_index("head")
    height = total.shape[0] // count
    for shift in range(count):
        first = pl.multiple_of(lax.rem(here + shift, count) * height, height)
        outs[shift][...] = total[pl.ds(first, height), :].astype(BF16)


def project_out(x, weight):
    count = lax.axis_size("head")
    chunks, per_dest, depth = x.shape
    rows = chunks * per_dest
    width = weight.shape[1]
    pieces = 8
    return pl.pallas_call(
        output_kernel,
        out_shape=[jax.ShapeDtypeStruct((rows // count, width), BF16)] * count,
        in_specs=[VMEM, HBM],
        out_specs=[VMEM] * count,
        scratch_shapes=[
            pltpu.VMEM((pieces, depth // pieces, width), BF16),
            pltpu.VMEM((rows, depth), F32),
            pltpu.VMEM((rows, width), F32),
            pltpu.SemaphoreType.DMA((pieces,)),
        ],
        compiler_params=params(weight.size * 2 + 10 * MIB),
        cost_estimate=cost(2 * rows * weight.size, weight.size * 2),
        name="output",
    )(x, weight)


def body(
    token_ids,
    suffix_lengths,
    embedding,
    attn_gain,
    qkv_weight,
    out_weight,
    prefix_keys,
    prefix_values,
    suffix_keys,
    suffix_values,
):
    steps, batch = token_ids.shape
    rows = steps * batch
    n_ctx = lax.axis_size("ctx")
    n_head = lax.axis_size("head")
    heads, block_context, head_dim = prefix_keys.shape
    width = embedding.shape[1]
    columns = qkv_weight.shape[2]
    group = columns * n_ctx // head_dim - 2
    step_index = jnp.arange(steps, dtype=jnp.int32)
    positions = block_context * n_ctx + suffix_lengths[:, None] + step_index[None, :]
    positions = positions.astype(F32).reshape(rows)
    half = head_dim // 2
    frequency = ROTARY_THETA ** (-2.0 * jnp.arange(half).astype(F32) / head_dim)
    angles = positions[:, None] * frequency
    cosine, sine = jnp.cos(angles), jnp.sin(angles)
    cosine = jnp.concatenate([cosine, cosine], axis=1)
    sine = jnp.concatenate([-sine, sine], axis=1)

    picked = lookup_rows(token_ids, embedding)
    joined = join_copies(exchange(picked, "ctx"))
    features = exchange(joined, "ctx")
    pieces = project(features, attn_gain, jnp.transpose(qkv_weight, (1, 2, 0)))
    pieces = send_pieces(pieces, "head")
    united = norm_copies(pieces, heads * columns, width * n_head)
    united = exchange(united, "ctx")
    packet, ready, fresh = attend(united, columns, cosine, sine, prefix_keys, prefix_values)
    parts = exchange(packet, "ctx")
    sums, maxima, totals = near(suffix_lengths, ready, fresh, suffix_keys, suffix_values)
    attention = merge_copies(parts, sums, maxima, totals, group, rows // n_ctx)
    attention = exchange(attention, "ctx")
    pieces = send_pieces(project_out(attention, out_weight), "head")
    result = pieces[0].astype(F32)
    for piece in pieces[1:]:
        result = result + piece.astype(F32)
    return result.astype(BF16).reshape(batch // n_head, steps, -1)


def solution(mesh):
    placed = (
        P(),
        P(),
        P("ctx", "head"),
        P("head"),
        P("head", None, "ctx"),
        P("head", "ctx"),
        P("head", "ctx", None),
        P("head", "ctx", None),
        P("ctx", None, "head", None),
        P("ctx", None, "head", None),
    )
    return jax.shard_map(
        body, mesh=mesh, in_specs=placed, out_specs=P("head", None, "ctx"), check_vma=False
    )
```

```python
import functools

import jax
import jax.numpy as jnp
from jax import lax
from jax.experimental import pallas as pl
from jax.experimental.pallas import tpu as pltpu
from jax.sharding import PartitionSpec as P

EPSILON = 1e-05
ROTARY_THETA = 500000.0
MASKED = -1e30
BF16 = jnp.bfloat16
F32 = jnp.float32
LANES = 128
MIB = 1 << 20
VMEM = pl.BlockSpec(memory_space=pltpu.VMEM)
SMEM = pl.BlockSpec(memory_space=pltpu.SMEM)
HBM = pl.BlockSpec(memory_space=pl.ANY)
NT = (((1,), (1,)), ((), ()))


def round_up(value, unit):
    return -(-value // unit) * unit


def params(limit):
    return pltpu.CompilerParams(vmem_limit_bytes=min(limit, 60 * MIB))


def cost(flops, moved, transcendentals=0):
    return pl.CostEstimate(flops=flops, bytes_accessed=moved, transcendentals=transcendentals)


def exchange(blocks, axis):
    return lax.all_to_all(blocks, axis, 0, 0)


def send_pieces(pieces, axis):
    count = lax.axis_size(axis)
    received = [pieces[0]]
    for shift in range(1, count):
        pairs = [(i, (i + shift) % count) for i in range(count)]
        received.append(lax.ppermute(pieces[shift], axis, pairs))
    return received


def lookup_kernel(tokens, table, out, blocks, rows_f32, sem):
    steps, batch = tokens.shape
    chunks, rows, width = out.shape
    local_rows = table.shape[0]
    base = lax.axis_index("ctx") * local_rows

    def place(row):
        offset = tokens[row % steps, row // steps] - base
        return offset, (offset >= 0) & (offset < local_rows)

    def copy(row, offset):
        start = pl.multiple_of((offset // 8) * 8, 8)
        return pltpu.make_async_copy(
            table.at[pl.ds(start, 8), :], blocks.at[row], sem.at[row]
        )

    for row in range(rows):
        offset, inside = place(row)

        @pl.when(inside)
        def _():
            copy(row, offset).start()

    rows_f32[...] = jnp.zeros_like(rows_f32)
    sublane = lax.broadcasted_iota(jnp.int32, (8, 1), 0)
    for row in range(rows):
        offset, inside = place(row)

        @pl.when(inside)
        def _():
            copy(row, offset).wait()
            picked = jnp.where(sublane == offset % 8, blocks[row].astype(F32), 0.0)
            rows_f32[row : row + 1, :] = jnp.sum(picked, axis=0, keepdims=True)

    for chunk in range(chunks):
        out[chunk] = rows_f32[:, chunk * width : (chunk + 1) * width].astype(BF16)


def lookup_rows(token_ids, embedding):
    steps, batch = token_ids.shape
    rows = steps * batch
    chunks = lax.axis_size("ctx")
    local_rows, width = embedding.shape
    if local_rows % 8 == 0:
        return pl.pallas_call(
            lookup_kernel,
            out_shape=jax.ShapeDtypeStruct((chunks, rows, width // chunks), BF16),
            in_specs=[SMEM, HBM],
            out_specs=VMEM,
            scratch_shapes=[
                pltpu.VMEM((rows, 8, width), BF16),
                pltpu.VMEM((rows, width), F32),
                pltpu.SemaphoreType.DMA((rows,)),
            ],
            compiler_params=params(6 * rows * width * 8),
            cost_estimate=cost(rows * width, rows * width * 16),
            name="lookup",
        )(token_ids, embedding)
    offsets = token_ids.T.reshape(rows) - lax.axis_index("ctx") * local_rows
    inside = (offsets >= 0) & (offsets < local_rows)
    picked = jnp.take(embedding, jnp.clip(offsets, 0, local_rows - 1), axis=0)
    picked = jnp.where(inside[:, None], picked, jnp.zeros((), BF16))
    return jnp.swapaxes(picked.reshape(rows, chunks, width // chunks), 0, 1)


def join_kernel(parts, out):
    total = parts[0].astype(F32)
    for source in range(1, parts.shape[0]):
        total = total + parts[source].astype(F32)
    joined = total.astype(BF16)
    for target in range(out.shape[0]):
        out[target] = joined


def join_copies(parts):
    return pl.pallas_call(
        join_kernel,
        out_shape=jax.ShapeDtypeStruct(parts.shape, BF16),
        in_specs=[VMEM],
        out_specs=VMEM,
        compiler_params=params(8 * MIB),
        name="join",
    )(parts)


def project_kernel(heads_here, x, gain, weight, *refs):
    count = weight.shape[0] // heads_here
    outs, scaled = refs[:count], refs[count]
    chunks, rows, chunk_width = x.shape
    columns = weight.shape[1]
    here = lax.axis_index("head")
    squares = jnp.zeros((rows, 1), F32)
    for chunk in range(chunks):
        span = slice(chunk * chunk_width, (chunk + 1) * chunk_width)
        features = x[chunk].astype(F32)
        squares = squares + jnp.sum(features * features, axis=-1, keepdims=True)
        scaled[:, span] = (features * gain[:, span]).astype(BF16)
    used = heads_here * columns
    rest = outs[0].shape[1] - used
    for shift in range(count):
        first = lax.rem(here + shift, count) * heads_here
        products = [
            lax.dot_general(scaled[...], weight[first + head], NT, preferred_element_type=F32)
            for head in range(heads_here)
        ]
        outs[shift][...] = jnp.concatenate(
            products + [jnp.broadcast_to(squares, (rows, rest))], axis=1
        )


def project(x, attn_gain, weight):
    count = lax.axis_size("head")
    chunks, rows, chunk_width = x.shape
    heads, columns, width = weight.shape
    heads_here = heads // count
    wide = round_up(heads_here * columns + 1, LANES)
    size = weight.size * 2
    return pl.pallas_call(
        functools.partial(project_kernel, heads_here),
        out_shape=[jax.ShapeDtypeStruct((rows, wide), F32)] * count,
        in_specs=[VMEM, VMEM, VMEM],
        out_specs=[VMEM] * count,
        scratch_shapes=[pltpu.VMEM((rows, width), BF16)],
        compiler_params=params(8 * MIB),
        cost_estimate=cost(2 * rows * weight.size, size),
        name="project",
    )(x, attn_gain.reshape(1, width), weight)


def norm_kernel(used, model_width, *refs):
    pieces, out = refs[:-1], refs[-1]
    total = pieces[0][...]
    for piece in pieces[1:]:
        total = total + piece[...]
    factor = lax.rsqrt(total[:, used : used + 1] * (1.0 / model_width) + EPSILON)
    united = (total * factor).astype(BF16)
    for target in range(out.shape[0]):
        out[target] = united


def norm_copies(pieces, used, model_width):
    rows, wide = pieces[0].shape
    return pl.pallas_call(
        functools.partial(norm_kernel, used, model_width),
        out_shape=jax.ShapeDtypeStruct((lax.axis_size("ctx"), rows, wide), BF16),
        in_specs=[VMEM] * len(pieces),
        out_specs=VMEM,
        compiler_params=params(8 * MIB),
        name="norm",
    )(*pieces)


def split3(value):
    first = value.astype(BF16).astype(F32)
    second = (value - first).astype(BF16).astype(F32)
    return first, second, value - first - second


def attend_kernel(columns, group, united, cosine, sine, keys, values, packet, ready, fresh, *scratch):
    query_buf, score_buf = scratch
    chunks, rows, _ = united.shape
    heads, context, head_dim = keys.shape
    per_dest = rows // chunks
    block = per_dest * group
    tile = min(512, context)
    tiles = context // tile

    cos = cosine[...]
    sin = sine[...]

    def rotated(vectors):
        return vectors * cos + pltpu.roll(vectors, head_dim // 2, 1) * sin

    for head in range(heads):
        first = head * columns
        whole = jnp.concatenate(
            [united[chunk].astype(F32)[:, first : first + columns] for chunk in range(chunks)],
            axis=1,
        )
        for j in range(group):
            query = rotated(whole[:, j * head_dim : (j + 1) * head_dim]) * head_dim ** (-0.5)
            for dest in range(chunks):
                start = dest * block + j * per_dest
                query_buf[head, start : start + per_dest, :] = query[
                    dest * per_dest : (dest + 1) * per_dest
                ]
        new_key = whole[:, group * head_dim : (group + 1) * head_dim]
        fresh[head] = rotated(new_key).astype(BF16)
        fresh[heads + head] = whole[:, (group + 1) * head_dim :].astype(BF16)

    lane = lax.broadcasted_iota(jnp.int32, (chunks * block, LANES), 1)
    for head in range(heads):
        query = query_buf[head].astype(BF16)
        for dest in range(chunks):
            ready[dest, head] = query[dest * block : (dest + 1) * block]
        highest = None
        for step in range(tiles):
            span = slice(step * tile, (step + 1) * tile)
            scores = lax.dot_general(
                query, keys[head, span, :], NT, preferred_element_type=F32
            )
            score_buf[:, span] = scores
            for part in range(tile // LANES):
                piece = scores[:, part * LANES : (part + 1) * LANES]
                highest = piece if highest is None else jnp.maximum(highest, piece)
        maxima = jnp.max(highest, axis=-1, keepdims=True)
        sums = jnp.zeros((chunks * block, head_dim), F32)
        totals = jnp.zeros((chunks * block, LANES), F32)
        for step in range(tiles):
            span = slice(step * tile, (step + 1) * tile)
            weights = jnp.exp(score_buf[:, span] - maxima).astype(BF16)
            sums = sums + jnp.dot(weights, values[head, span, :], preferred_element_type=F32)
            wide = weights.astype(F32)
            for part in range(tile // LANES):
                totals = totals + wide[:, part * LANES : (part + 1) * LANES]
        total = jnp.sum(totals, axis=-1, keepdims=True)
        table = jnp.zeros((chunks * block, LANES), F32)
        for index, piece in enumerate(split3(maxima) + split3(total)):
            table = jnp.where(lane == index, piece, table)
        rounded = sums.astype(BF16)
        for dest in range(chunks):
            packet[dest, head * block : (head + 1) * block] = rounded[
                dest * block : (dest + 1) * block
            ]
        turned = jnp.transpose(table)[:16]
        for dest in range(chunks):
            packet[dest, heads * block + head * 16 : heads * block + (head + 1) * 16, :block] = turned[
                :, dest * block : (dest + 1) * block
            ].astype(BF16)


def attend(united, columns, cosine, sine, keys, values):
    chunks, rows, _ = united.shape
    heads, context, head_dim = keys.shape
    group = columns * chunks // head_dim - 2
    block = rows // chunks * group
    size = keys.size * 2
    flat = chunks * block
    return pl.pallas_call(
        functools.partial(attend_kernel, columns, group),
        out_shape=[
            jax.ShapeDtypeStruct((chunks, heads * (block + 16), head_dim), BF16),
            jax.ShapeDtypeStruct((chunks, heads, block, head_dim), BF16),
            jax.ShapeDtypeStruct((2 * heads, rows, head_dim), BF16),
        ],
        in_specs=[VMEM] * 5,
        out_specs=[VMEM] * 3,
        scratch_shapes=[
            pltpu.VMEM((heads, flat, head_dim), F32),
            pltpu.VMEM((flat, context), F32),
        ],
        compiler_params=params(flat * context * 4 + 12 * MIB),
        cost_estimate=cost(4 * heads * flat * context * head_dim, 2 * size, heads * flat * context),
        name="attend",
    )(united, cosine, sine, keys, values)


def near_kernel(owned, lengths, ready, fresh, keys, values, sums, maxima, totals):
    heads, rows, head_dim = fresh.shape
    heads //= 2
    _, _, block, _ = ready.shape
    slots_all = keys.shape[1]
    per_dest = rows // ready.shape[0]
    steps = per_dest // owned
    mine = lax.axis_index("ctx")

    def iota(shape, axis):
        return lax.broadcasted_iota(jnp.int32, shape, axis)

    query_place = iota((block, 1), 0) % per_dest
    sequence = query_place // steps
    step = query_place % steps
    slot = iota((1, slots_all), 1)
    fresh_row = iota((1, rows), 1)
    fresh_here = (fresh_row // steps == mine * owned + sequence) & (fresh_row % steps <= step)
    for head in range(heads):
        query = ready[mine, head]
        fresh_scores = lax.dot_general(query, fresh[head], NT, preferred_element_type=F32)
        fresh_scores = jnp.where(fresh_here, fresh_scores, MASKED)
        scores = []
        highest = jnp.max(fresh_scores, axis=-1, keepdims=True)
        for s in range(owned):
            found = lax.dot_general(query, keys[s], NT, preferred_element_type=F32)
            live = (sequence == s) & (slot % heads == head)
            live = live & (slot // heads < lengths[mine * owned + s])
            found = jnp.where(live, found, MASKED)
            scores.append(found)
            highest = jnp.maximum(highest, jnp.max(found, axis=-1, keepdims=True))
        weights = jnp.exp(fresh_scores - highest).astype(BF16)
        total = jnp.sum(weights.astype(F32), axis=-1, keepdims=True)
        result = jnp.dot(weights, fresh[heads + head], preferred_element_type=F32)
        for s in range(owned):
            weights = jnp.exp(scores[s] - highest).astype(BF16)
            total = total + jnp.sum(weights.astype(F32), axis=-1, keepdims=True)
            result = result + jnp.dot(weights, values[s], preferred_element_type=F32)
        span = slice(head * block, (head + 1) * block)
        sums[span, :] = result
        maxima[span, :] = jnp.broadcast_to(highest, (block, head_dim))
        totals[span, :] = jnp.broadcast_to(total, (block, head_dim))


def near(lengths, ready, fresh, keys, values):
    owned, slots, heads, head_dim = keys.shape
    block = ready.shape[2]
    shape = jax.ShapeDtypeStruct((heads * block, head_dim), F32)
    return pl.pallas_call(
        functools.partial(near_kernel, owned),
        out_shape=[shape] * 3,
        in_specs=[SMEM, VMEM, VMEM, VMEM, VMEM],
        out_specs=[VMEM] * 3,
        compiler_params=params(8 * MIB),
        cost_estimate=cost(4 * heads * block * owned * slots * heads * head_dim, keys.size * 4),
        name="near",
    )(
        lengths,
        ready,
        fresh,
        keys.reshape(owned, slots * heads, head_dim),
        values.reshape(owned, slots * heads, head_dim),
    )


def merge_kernel(group, parts, near_sums, near_maxima, near_totals, out, places, stats):
    chunks = parts.shape[0]
    per_dest = out.shape[1]
    block = per_dest * group
    queries, head_dim = near_sums.shape
    heads = queries // block
    highest = near_maxima[...][:, :1]
    maxima, totals = [], []
    for source in range(chunks):
        for head in range(heads):
            low = queries + head * 16
            found = parts[source, low : low + 16, :].astype(F32)[:8]
            row = (source * heads + head) * 8
            stats[row : row + 8, :] = found
    turned = jnp.transpose(stats[...])[:block]
    for source in range(chunks):
        m, t = [], []
        for head in range(heads):
            column = (source * heads + head) * 8
            get = lambda k: turned[:, column + k : column + k + 1]
            m.append(get(0) + get(1) + get(2))
            t.append(get(3) + get(4) + get(5))
        maxima.append(jnp.concatenate(m, axis=0))
        totals.append(jnp.concatenate(t, axis=0))
        highest = jnp.maximum(highest, maxima[-1])
    scale = jnp.exp(near_maxima[...][:, :1] - highest)
    numerator = near_sums[...] * scale
    denominator = near_totals[...][:, :1] * scale
    for source in range(chunks):
        scale = jnp.exp(maxima[source] - highest)
        numerator = numerator + parts[source, :queries, :].astype(F32) * scale
        denominator = denominator + totals[source] * scale
    attention = numerator / denominator
    for index in range(heads * group):
        places[:, index * head_dim : (index + 1) * head_dim] = attention[
            index * per_dest : (index + 1) * per_dest
        ]
    rounded = places[...].astype(BF16)
    for target in range(chunks):
        out[target] = rounded


def merge_copies(parts, sums, maxima, totals, group, per_dest):
    chunks = parts.shape[0]
    queries, head_dim = sums.shape
    heads = queries // (per_dest * group)
    width = heads * group * head_dim
    return pl.pallas_call(
        functools.partial(merge_kernel, group),
        out_shape=jax.ShapeDtypeStruct((chunks, per_dest, width), BF16),
        in_specs=[VMEM] * 4,
        out_specs=VMEM,
        scratch_shapes=[
            pltpu.VMEM((per_dest, width), F32),
            pltpu.VMEM((chunks * heads * 8, head_dim), F32),
        ],
        compiler_params=params(12 * MIB),
        name="merge",
    )(parts, sums, maxima, totals)


def output_kernel(x, weight, *refs):
    chunks, per_dest, depth = x.shape
    rows_f32, total = refs[-2:]
    outs = refs[:-2]
    count = len(outs)
    for chunk in range(chunks):
        rows_f32[chunk * per_dest : (chunk + 1) * per_dest, :] = x[chunk].astype(F32)
    total[...] = jnp.dot(
        rows_f32[...].astype(BF16), weight[...], preferred_element_type=F32
    )
    here = lax.axis_index("head")
    height = total.shape[0] // count
    for shift in range(count):
        first = pl.multiple_of(lax.rem(here + shift, count) * height, height)
        outs[shift][...] = total[pl.ds(first, height), :].astype(BF16)


def project_out(x, weight):
    count = lax.axis_size("head")
    chunks, per_dest, depth = x.shape
    rows = chunks * per_dest
    width = weight.shape[1]
    return pl.pallas_call(
        output_kernel,
        out_shape=[jax.ShapeDtypeStruct((rows // count, width), BF16)] * count,
        in_specs=[VMEM, VMEM],
        out_specs=[VMEM] * count,
        scratch_shapes=[pltpu.VMEM((rows, depth), F32), pltpu.VMEM((rows, width), F32)],
        compiler_params=params(8 * MIB),
        cost_estimate=cost(2 * rows * weight.size, weight.size * 2),
        name="output",
    )(x, weight)


def body(
    token_ids,
    suffix_lengths,
    embedding,
    attn_gain,
    qkv_weight,
    out_weight,
    prefix_keys,
    prefix_values,
    suffix_keys,
    suffix_values,
):
    steps, batch = token_ids.shape
    rows = steps * batch
    n_ctx = lax.axis_size("ctx")
    n_head = lax.axis_size("head")
    heads, block_context, head_dim = prefix_keys.shape
    width = embedding.shape[1]
    columns = qkv_weight.shape[2]
    group = columns * n_ctx // head_dim - 2
    step_index = jnp.arange(steps, dtype=jnp.int32)
    positions = block_context * n_ctx + suffix_lengths[:, None] + step_index[None, :]
    positions = positions.astype(F32).reshape(rows)
    half = head_dim // 2
    frequency = ROTARY_THETA ** (-2.0 * jnp.arange(half).astype(F32) / head_dim)
    angles = positions[:, None] * frequency
    cosine, sine = jnp.cos(angles), jnp.sin(angles)
    cosine = jnp.concatenate([cosine, cosine], axis=1)
    sine = jnp.concatenate([-sine, sine], axis=1)

    token_ids, cosine, sine = lax.optimization_barrier((token_ids, cosine, sine))
    picked = lookup_rows(token_ids, embedding)
    joined = join_copies(exchange(picked, "ctx"))
    features = exchange(joined, "ctx")
    pieces = project(features, attn_gain, jnp.transpose(qkv_weight, (1, 2, 0)))
    pieces = send_pieces(pieces, "head")
    united = norm_copies(pieces, heads * columns, width * n_head)
    united = exchange(united, "ctx")
    packet, ready, fresh = attend(united, columns, cosine, sine, prefix_keys, prefix_values)
    sums, maxima, totals = near(suffix_lengths, ready, fresh, suffix_keys, suffix_values)
    packet, sums, maxima, totals = lax.optimization_barrier((packet, sums, maxima, totals))
    parts = exchange(packet, "ctx")
    attention = merge_copies(parts, sums, maxima, totals, group, rows // n_ctx)
    attention = exchange(attention, "ctx")
    pieces = send_pieces(project_out(attention, out_weight), "head")
    result = pieces[0].astype(F32)
    for piece in pieces[1:]:
        result = result + piece.astype(F32)
    return result.astype(BF16).reshape(batch // n_head, steps, -1)


def solution(mesh):
    placed = (
        P(),
        P(),
        P("ctx", "head"),
        P("head"),
        P("head", None, "ctx"),
        P("head", "ctx"),
        P("head", "ctx", None),
        P("head", "ctx", None),
        P("ctx", None, "head", None),
        P("ctx", None, "head", None),
    )
    return jax.shard_map(
        body, mesh=mesh, in_specs=placed, out_specs=P("head", None, "ctx"), check_vma=False
    )
```

```python
import functools

import jax
import jax.numpy as jnp
from jax import lax
from jax.experimental import pallas as pl
from jax.experimental.pallas import tpu as pltpu
from jax.sharding import PartitionSpec as P

EPSILON = 1e-05
ROTARY_THETA = 500000.0
MASKED = -1e30
BF16 = jnp.bfloat16
F32 = jnp.float32
LANES = 128
MIB = 1 << 20
VMEM = pl.BlockSpec(memory_space=pltpu.VMEM)
SMEM = pl.BlockSpec(memory_space=pltpu.SMEM)
HBM = pl.BlockSpec(memory_space=pl.ANY)
NT = (((1,), (1,)), ((), ()))


def round_up(value, unit):
    return -(-value // unit) * unit


def params(limit):
    return pltpu.CompilerParams(vmem_limit_bytes=min(limit, 60 * MIB))


def cost(flops, moved, transcendentals=0):
    return pl.CostEstimate(flops=flops, bytes_accessed=moved, transcendentals=transcendentals)


def exchange(blocks, axis):
    return lax.all_to_all(blocks, axis, 0, 0)


def send_pieces(pieces, axis):
    count = lax.axis_size(axis)
    received = [pieces[0]]
    for shift in range(1, count):
        pairs = [(i, (i + shift) % count) for i in range(count)]
        received.append(lax.ppermute(pieces[shift], axis, pairs))
    return received


def token_at(tokens, row):
    steps = tokens.shape[0]
    return tokens[row % steps, row // steps]


def assign_slots(tokens, rows, owners, local_rows, capacity):
    lanes = round_up(rows, LANES)
    down = lax.broadcasted_iota(jnp.int32, (rows, lanes), 0)
    across = lax.broadcasted_iota(jnp.int32, (rows, lanes), 1)
    column = jnp.zeros((rows, lanes), jnp.int32)
    line = jnp.full((rows, lanes), -1, jnp.int32)
    for row in range(rows):
        token = token_at(tokens, row)
        column = jnp.where(down == row, token, column)
        line = jnp.where(across == row, token, line)
    owner_column = jnp.zeros((rows, lanes), F32)
    owner_line = jnp.zeros((rows, lanes), F32)
    for owner in range(1, owners):
        owner_column += jnp.where(column >= owner * local_rows, 1.0, 0.0)
        owner_line += jnp.where(line >= owner * local_rows, 1.0, 0.0)
    same = jnp.where(column == line, 1.0, 0.0)
    index = across.astype(F32)
    earliest = jnp.min(jnp.where(same > 0, index, float(lanes)), axis=1, keepdims=True)
    repeated = jnp.max(jnp.where(down < across, same, 0.0), axis=0, keepdims=True)
    counted = jnp.where((repeated == 0) & (across < rows) & (index < earliest), 1.0, 0.0)
    slot = jnp.sum(jnp.where(owner_column == owner_line, counted, 0.0), axis=1, keepdims=True)
    place = jnp.where(slot < capacity, owner_column[:, :1] * capacity + slot, -1.0)
    first = earliest == down[:, :1].astype(F32)
    return place, first


def fetch_rows(tokens, table, blocks, rows_f32, sem, between=None):
    rows = rows_f32.shape[0]
    local_rows = table.shape[0]
    base = lax.axis_index("ctx") * local_rows

    def find(row):
        offset = token_at(tokens, row) - base
        return offset, (offset >= 0) & (offset < local_rows)

    def copy(row, offset):
        start = pl.multiple_of((offset // 8) * 8, 8)
        return pltpu.make_async_copy(
            table.at[pl.ds(start, 8), :], blocks.at[row], sem.at[row]
        )

    for row in range(rows):
        offset, inside = find(row)

        @pl.when(inside)
        def _():
            copy(row, offset).start()

    rows_f32[...] = jnp.zeros_like(rows_f32)
    result = None if between is None else between()
    sublane = lax.broadcasted_iota(jnp.int32, (8, 1), 0)
    for row in range(rows):
        offset, inside = find(row)

        @pl.when(inside)
        def _():
            copy(row, offset).wait()
            picked = jnp.where(sublane == offset % 8, blocks[row].astype(F32), 0.0)
            rows_f32[row : row + 1, :] = jnp.sum(picked, axis=0, keepdims=True)

    return result


def lookup_kernel(owners, tokens, table, packed, places, crowded, blocks, rows_f32, sem):
    capacity, _ = packed.shape
    rows = rows_f32.shape[0]

    def between():
        return assign_slots(tokens, rows, owners, table.shape[0], capacity)

    place, first = fetch_rows(tokens, table, blocks, rows_f32, sem, between)
    places[...] = jnp.broadcast_to(place, places.shape)
    crowded[0] = jnp.max(jnp.where(place < 0, 1, 0))
    slot = lax.broadcasted_iota(jnp.int32, (rows, capacity), 1) + lax.axis_index("ctx") * capacity
    chosen = jnp.where((place == slot.astype(F32)) & first, 1.0, 0.0).astype(BF16)
    packed[...] = lax.dot_general(
        chosen, rows_f32[...].astype(BF16), (((0,), (0,)), ((), ())), preferred_element_type=F32
    ).astype(BF16)


def rest_kernel(tokens, places, table, out, blocks, rows_f32, sem):
    chunks, rows, width = out.shape
    fetch_rows(tokens, table, blocks, rows_f32, sem)
    left = places[...][:, :1] < 0
    for chunk in range(chunks):
        found = rows_f32[:, chunk * width : (chunk + 1) * width]
        out[chunk] = jnp.where(left, found, 0.0).astype(BF16)


def fetch_scratch(rows, width):
    return [
        pltpu.VMEM((rows, 8, width), BF16),
        pltpu.VMEM((rows, width), F32),
        pltpu.SemaphoreType.DMA((rows,)),
    ]


def spread_kernel(block, first, out):
    for target in range(out.shape[0]):
        out[target] = block[...]


def spread(block, first, hint):
    count = lax.axis_size("ctx")
    return pl.pallas_call(
        spread_kernel,
        out_shape=jax.ShapeDtypeStruct((count,) + block.shape, block.dtype),
        in_specs=[VMEM, HBM],
        out_specs=VMEM,
        compiler_params=params(8 * MIB),
        cost_estimate=cost(400 * hint, hint),
        name="spread",
    )(block, first)


def lookup_packed(token_ids, embedding, capacity):
    steps, batch = token_ids.shape
    rows = steps * batch
    owners = lax.axis_size("ctx")
    _, width = embedding.shape
    return pl.pallas_call(
        functools.partial(lookup_kernel, owners),
        out_shape=[
            jax.ShapeDtypeStruct((capacity, width), BF16),
            jax.ShapeDtypeStruct((rows, LANES), F32),
            jax.ShapeDtypeStruct((1,), jnp.int32),
        ],
        in_specs=[SMEM, HBM],
        out_specs=[VMEM, VMEM, SMEM],
        scratch_shapes=fetch_scratch(rows, width),
        compiler_params=params(6 * rows * width * 8),
        cost_estimate=cost(rows * width, rows * width * 16),
        name="lookup",
    )(token_ids, embedding)


def lookup_rest(token_ids, places, embedding):
    rows = places.shape[0]
    chunks = lax.axis_size("ctx")
    _, width = embedding.shape
    return pl.pallas_call(
        rest_kernel,
        out_shape=jax.ShapeDtypeStruct((chunks, rows, width // chunks), BF16),
        in_specs=[SMEM, VMEM, HBM],
        out_specs=VMEM,
        scratch_shapes=fetch_scratch(rows, width),
        compiler_params=params(6 * rows * width * 8),
        name="rest",
    )(token_ids, places, embedding)


def lookup_all(token_ids, embedding):
    steps, batch = token_ids.shape
    rows = steps * batch
    chunks = lax.axis_size("ctx")
    local_rows, width = embedding.shape
    offsets = token_ids.T.reshape(rows) - lax.axis_index("ctx") * local_rows
    inside = (offsets >= 0) & (offsets < local_rows)
    picked = jnp.take(embedding, jnp.clip(offsets, 0, local_rows - 1), axis=0)
    picked = jnp.where(inside[:, None], picked, jnp.zeros((), BF16))
    return jnp.swapaxes(picked.reshape(rows, chunks, width // chunks), 0, 1)


def join_kernel(parts, out):
    total = parts[0].astype(F32)
    for source in range(1, parts.shape[0]):
        total = total + parts[source].astype(F32)
    joined = total.astype(BF16)
    for target in range(out.shape[0]):
        out[target] = joined


def join_copies(parts):
    return pl.pallas_call(
        join_kernel,
        out_shape=jax.ShapeDtypeStruct(parts.shape, BF16),
        in_specs=[VMEM],
        out_specs=VMEM,
        compiler_params=params(8 * MIB),
        name="join",
    )(parts)


def project_kernel(heads_here, packed, x, gain, weight, *refs):
    if packed:
        slots, places, *refs = refs
    count = weight.shape[0] // heads_here
    outs, scaled = refs[:count], refs[count]
    chunks, rows, chunk_width = x.shape
    if packed:
        owners, capacity, width = slots.shape
        held = slots[...].astype(F32).reshape(owners * capacity, width).astype(BF16)
        slot = lax.broadcasted_iota(jnp.int32, (rows, owners * capacity), 1).astype(F32)
        chosen = jnp.where(places[...][:, :1] == slot, 1.0, 0.0).astype(BF16)
    columns = weight.shape[1]
    here = lax.axis_index("head")
    squares = jnp.zeros((rows, 1), F32)
    for chunk in range(chunks):
        span = slice(chunk * chunk_width, (chunk + 1) * chunk_width)
        features = x[chunk].astype(F32)
        if packed:
            features += jnp.dot(chosen, held[:, span], preferred_element_type=F32)
        squares = squares + jnp.sum(features * features, axis=-1, keepdims=True)
        scaled[:, span] = (features * gain[:, span]).astype(BF16)
    used = heads_here * columns
    rest = outs[0].shape[1] - used
    for shift in range(count):
        first = lax.rem(here + shift, count) * heads_here
        products = [
            lax.dot_general(scaled[...], weight[first + head], NT, preferred_element_type=F32)
            for head in range(heads_here)
        ]
        outs[shift][...] = jnp.concatenate(
            products + [jnp.broadcast_to(squares, (rows, rest))], axis=1
        )


def project(x, attn_gain, weight, packed=()):
    count = lax.axis_size("head")
    chunks, rows, chunk_width = x.shape
    heads, columns, width = weight.shape
    heads_here = heads // count
    wide = round_up(heads_here * columns + 1, LANES)
    size = weight.size * 2
    return pl.pallas_call(
        functools.partial(project_kernel, heads_here, bool(packed)),
        out_shape=[jax.ShapeDtypeStruct((rows, wide), F32)] * count,
        in_specs=[VMEM] * (3 + len(packed)),
        out_specs=[VMEM] * count,
        scratch_shapes=[pltpu.VMEM((rows, width), BF16)],
        compiler_params=params(8 * MIB),
        cost_estimate=cost(2 * rows * weight.size, size),
        name="project",
    )(x, attn_gain.reshape(1, width), weight, *packed)


def norm_kernel(used, model_width, *refs):
    pieces, out = refs[:-1], refs[-1]
    total = pieces[0][...]
    for piece in pieces[1:]:
        total = total + piece[...]
    factor = lax.rsqrt(total[:, used : used + 1] * (1.0 / model_width) + EPSILON)
    united = (total * factor).astype(BF16)
    for target in range(out.shape[0]):
        out[target] = united


def norm_copies(pieces, used, model_width):
    rows, wide = pieces[0].shape
    return pl.pallas_call(
        functools.partial(norm_kernel, used, model_width),
        out_shape=jax.ShapeDtypeStruct((lax.axis_size("ctx"), rows, wide), BF16),
        in_specs=[VMEM] * len(pieces),
        out_specs=VMEM,
        compiler_params=params(8 * MIB),
        name="norm",
    )(*pieces)


def split3(value):
    first = value.astype(BF16).astype(F32)
    second = (value - first).astype(BF16).astype(F32)
    return first, second, value - first - second


def attend_kernel(columns, group, united, cosine, sine, keys, values, packet, ready, fresh, *scratch):
    query_buf, score_buf = scratch
    chunks, rows, _ = united.shape
    heads, context, head_dim = keys.shape
    per_dest = rows // chunks
    block = per_dest * group
    tile = min(512, context)
    tiles = context // tile

    cos = cosine[...]
    sin = sine[...]

    def rotated(vectors):
        return vectors * cos + pltpu.roll(vectors, head_dim // 2, 1) * sin

    for head in range(heads):
        first = head * columns
        whole = jnp.concatenate(
            [united[chunk].astype(F32)[:, first : first + columns] for chunk in range(chunks)],
            axis=1,
        )
        for j in range(group):
            query = rotated(whole[:, j * head_dim : (j + 1) * head_dim]) * head_dim ** (-0.5)
            for dest in range(chunks):
                start = dest * block + j * per_dest
                query_buf[head, start : start + per_dest, :] = query[
                    dest * per_dest : (dest + 1) * per_dest
                ]
        new_key = whole[:, group * head_dim : (group + 1) * head_dim]
        fresh[head] = rotated(new_key).astype(BF16)
        fresh[heads + head] = whole[:, (group + 1) * head_dim :].astype(BF16)

    lane = lax.broadcasted_iota(jnp.int32, (chunks * block, LANES), 1)
    for head in range(heads):
        query = query_buf[head].astype(BF16)
        for dest in range(chunks):
            ready[dest, head] = query[dest * block : (dest + 1) * block]
        highest = None
        for step in range(tiles):
            span = slice(step * tile, (step + 1) * tile)
            scores = lax.dot_general(
                query, keys[head, span, :], NT, preferred_element_type=F32
            )
            score_buf[:, span] = scores
            for part in range(tile // LANES):
                piece = scores[:, part * LANES : (part + 1) * LANES]
                highest = piece if highest is None else jnp.maximum(highest, piece)
        maxima = jnp.max(highest, axis=-1, keepdims=True)
        sums = jnp.zeros((chunks * block, head_dim), F32)
        totals = jnp.zeros((chunks * block, LANES), F32)
        for step in range(tiles):
            span = slice(step * tile, (step + 1) * tile)
            weights = jnp.exp(score_buf[:, span] - maxima).astype(BF16)
            sums = sums + jnp.dot(weights, values[head, span, :], preferred_element_type=F32)
            wide = weights.astype(F32)
            for part in range(tile // LANES):
                totals = totals + wide[:, part * LANES : (part + 1) * LANES]
        total = jnp.sum(totals, axis=-1, keepdims=True)
        table = jnp.zeros((chunks * block, LANES), F32)
        for index, piece in enumerate(split3(maxima) + split3(total)):
            table = jnp.where(lane == index, piece, table)
        rounded = sums.astype(BF16)
        for dest in range(chunks):
            packet[dest, head * block : (head + 1) * block] = rounded[
                dest * block : (dest + 1) * block
            ]
        turned = jnp.transpose(table)[:16]
        for dest in range(chunks):
            packet[dest, heads * block + head * 16 : heads * block + (head + 1) * 16, :block] = turned[
                :, dest * block : (dest + 1) * block
            ].astype(BF16)


def attend(united, columns, cosine, sine, keys, values):
    chunks, rows, _ = united.shape
    heads, context, head_dim = keys.shape
    group = columns * chunks // head_dim - 2
    block = rows // chunks * group
    size = keys.size * 2
    flat = chunks * block
    return pl.pallas_call(
        functools.partial(attend_kernel, columns, group),
        out_shape=[
            jax.ShapeDtypeStruct((chunks, heads * (block + 16), head_dim), BF16),
            jax.ShapeDtypeStruct((chunks, heads, block, head_dim), BF16),
            jax.ShapeDtypeStruct((2 * heads, rows, head_dim), BF16),
        ],
        in_specs=[VMEM] * 5,
        out_specs=[VMEM] * 3,
        scratch_shapes=[
            pltpu.VMEM((heads, flat, head_dim), F32),
            pltpu.VMEM((flat, context), F32),
        ],
        compiler_params=params(flat * context * 4 + 12 * MIB),
        cost_estimate=cost(4 * heads * flat * context * head_dim, 2 * size, heads * flat * context),
        name="attend",
    )(united, cosine, sine, keys, values)


def near_kernel(owned, lengths, ready, fresh, keys, values, sums, maxima, totals):
    heads, rows, head_dim = fresh.shape
    heads //= 2
    _, _, block, _ = ready.shape
    slots_all = keys.shape[1]
    per_dest = rows // ready.shape[0]
    steps = per_dest // owned
    mine = lax.axis_index("ctx")

    def iota(shape, axis):
        return lax.broadcasted_iota(jnp.int32, shape, axis)

    query_place = iota((block, 1), 0) % per_dest
    sequence = query_place // steps
    step = query_place % steps
    slot = iota((1, slots_all), 1)
    fresh_row = iota((1, rows), 1)
    fresh_here = (fresh_row // steps == mine * owned + sequence) & (fresh_row % steps <= step)
    for head in range(heads):
        query = ready[mine, head]
        fresh_scores = lax.dot_general(query, fresh[head], NT, preferred_element_type=F32)
        fresh_scores = jnp.where(fresh_here, fresh_scores, MASKED)
        scores = []
        highest = jnp.max(fresh_scores, axis=-1, keepdims=True)
        for s in range(owned):
            found = lax.dot_general(query, keys[s], NT, preferred_element_type=F32)
            live = (sequence == s) & (slot % heads == head)
            live = live & (slot // heads < lengths[mine * owned + s])
            found = jnp.where(live, found, MASKED)
            scores.append(found)
            highest = jnp.maximum(highest, jnp.max(found, axis=-1, keepdims=True))
        weights = jnp.exp(fresh_scores - highest).astype(BF16)
        total = jnp.sum(weights.astype(F32), axis=-1, keepdims=True)
        result = jnp.dot(weights, fresh[heads + head], preferred_element_type=F32)
        for s in range(owned):
            weights = jnp.exp(scores[s] - highest).astype(BF16)
            total = total + jnp.sum(weights.astype(F32), axis=-1, keepdims=True)
            result = result + jnp.dot(weights, values[s], preferred_element_type=F32)
        span = slice(head * block, (head + 1) * block)
        sums[span, :] = result
        maxima[span, :] = jnp.broadcast_to(highest, (block, head_dim))
        totals[span, :] = jnp.broadcast_to(total, (block, head_dim))


def near(lengths, ready, fresh, keys, values):
    owned, slots, heads, head_dim = keys.shape
    block = ready.shape[2]
    shape = jax.ShapeDtypeStruct((heads * block, head_dim), F32)
    return pl.pallas_call(
        functools.partial(near_kernel, owned),
        out_shape=[shape] * 3,
        in_specs=[SMEM, VMEM, VMEM, VMEM, VMEM],
        out_specs=[VMEM] * 3,
        compiler_params=params(8 * MIB),
        cost_estimate=cost(4 * heads * block * owned * slots * heads * head_dim, keys.size * 4),
        name="near",
    )(
        lengths,
        ready,
        fresh,
        keys.reshape(owned, slots * heads, head_dim),
        values.reshape(owned, slots * heads, head_dim),
    )


def merge_kernel(group, parts, near_sums, near_maxima, near_totals, out, places, stats):
    chunks = parts.shape[0]
    per_dest = out.shape[1]
    block = per_dest * group
    queries, head_dim = near_sums.shape
    heads = queries // block
    highest = near_maxima[...][:, :1]
    maxima, totals = [], []
    for source in range(chunks):
        for head in range(heads):
            low = queries + head * 16
            found = parts[source, low : low + 16, :].astype(F32)[:8]
            row = (source * heads + head) * 8
            stats[row : row + 8, :] = found
    turned = jnp.transpose(stats[...])[:block]
    for source in range(chunks):
        m, t = [], []
        for head in range(heads):
            column = (source * heads + head) * 8
            get = lambda k: turned[:, column + k : column + k + 1]
            m.append(get(0) + get(1) + get(2))
            t.append(get(3) + get(4) + get(5))
        maxima.append(jnp.concatenate(m, axis=0))
        totals.append(jnp.concatenate(t, axis=0))
        highest = jnp.maximum(highest, maxima[-1])
    scale = jnp.exp(near_maxima[...][:, :1] - highest)
    numerator = near_sums[...] * scale
    denominator = near_totals[...][:, :1] * scale
    for source in range(chunks):
        scale = jnp.exp(maxima[source] - highest)
        numerator = numerator + parts[source, :queries, :].astype(F32) * scale
        denominator = denominator + totals[source] * scale
    attention = numerator / denominator
    for index in range(heads * group):
        places[:, index * head_dim : (index + 1) * head_dim] = attention[
            index * per_dest : (index + 1) * per_dest
        ]
    rounded = places[...].astype(BF16)
    for target in range(chunks):
        out[target] = rounded


def merge_copies(parts, sums, maxima, totals, group, per_dest):
    chunks = parts.shape[0]
    queries, head_dim = sums.shape
    heads = queries // (per_dest * group)
    width = heads * group * head_dim
    return pl.pallas_call(
        functools.partial(merge_kernel, group),
        out_shape=jax.ShapeDtypeStruct((chunks, per_dest, width), BF16),
        in_specs=[VMEM] * 4,
        out_specs=VMEM,
        scratch_shapes=[
            pltpu.VMEM((per_dest, width), F32),
            pltpu.VMEM((chunks * heads * 8, head_dim), F32),
        ],
        compiler_params=params(12 * MIB),
        name="merge",
    )(parts, sums, maxima, totals)


def output_kernel(x, weight, *refs):
    chunks, per_dest, depth = x.shape
    rows_f32, total = refs[-2:]
    outs = refs[:-2]
    count = len(outs)
    for chunk in range(chunks):
        rows_f32[chunk * per_dest : (chunk + 1) * per_dest, :] = x[chunk].astype(F32)
    total[...] = jnp.dot(
        rows_f32[...].astype(BF16), weight[...], preferred_element_type=F32
    )
    here = lax.axis_index("head")
    height = total.shape[0] // count
    for shift in range(count):
        first = pl.multiple_of(lax.rem(here + shift, count) * height, height)
        outs[shift][...] = total[pl.ds(first, height), :].astype(BF16)


def project_out(x, weight):
    count = lax.axis_size("head")
    chunks, per_dest, depth = x.shape
    rows = chunks * per_dest
    width = weight.shape[1]
    return pl.pallas_call(
        output_kernel,
        out_shape=[jax.ShapeDtypeStruct((rows // count, width), BF16)] * count,
        in_specs=[VMEM, VMEM],
        out_specs=[VMEM] * count,
        scratch_shapes=[pltpu.VMEM((rows, depth), F32), pltpu.VMEM((rows, width), F32)],
        compiler_params=params(8 * MIB),
        cost_estimate=cost(2 * rows * weight.size, weight.size * 2),
        name="output",
    )(x, weight)


def body(
    token_ids,
    suffix_lengths,
    embedding,
    attn_gain,
    qkv_weight,
    out_weight,
    prefix_keys,
    prefix_values,
    suffix_keys,
    suffix_values,
):
    steps, batch = token_ids.shape
    rows = steps * batch
    n_ctx = lax.axis_size("ctx")
    n_head = lax.axis_size("head")
    heads, block_context, head_dim = prefix_keys.shape
    width = embedding.shape[1]
    columns = qkv_weight.shape[2]
    group = columns * n_ctx // head_dim - 2
    step_index = jnp.arange(steps, dtype=jnp.int32)
    positions = block_context * n_ctx + suffix_lengths[:, None] + step_index[None, :]
    positions = positions.astype(F32).reshape(rows)
    half = head_dim // 2
    frequency = ROTARY_THETA ** (-2.0 * jnp.arange(half).astype(F32) / head_dim)
    angles = positions[:, None] * frequency
    cosine, sine = jnp.cos(angles), jnp.sin(angles)
    cosine = jnp.concatenate([cosine, cosine], axis=1)
    sine = jnp.concatenate([-sine, sine], axis=1)

    token_ids, cosine, sine = lax.optimization_barrier((token_ids, cosine, sine))
    capacity = 2 * rows // n_ctx
    qkv_weight = jnp.transpose(qkv_weight, (1, 2, 0))
    if embedding.shape[0] % 8 == 0 and capacity % 8 == 0:
        packed, places, crowded = lookup_packed(token_ids, embedding, capacity)

        def rest():
            found = lookup_rest(token_ids, places, embedding)
            return exchange(join_copies(exchange(found, "ctx")), "ctx")

        def nothing():
            return jnp.zeros((n_ctx, rows, width // n_ctx), BF16)

        features = lax.cond(crowded[0] > 0, rest, nothing)
        packed = exchange(spread(packed, features, 4 * qkv_weight.size), "ctx")
        pieces = project(features, attn_gain, qkv_weight, (packed, places))
    else:
        joined = join_copies(exchange(lookup_all(token_ids, embedding), "ctx"))
        pieces = project(exchange(joined, "ctx"), attn_gain, qkv_weight)
    pieces = send_pieces(pieces, "head")
    united = norm_copies(pieces, heads * columns, width * n_head)
    united = exchange(united, "ctx")
    packet, ready, fresh = attend(united, columns, cosine, sine, prefix_keys, prefix_values)
    sums, maxima, totals = near(suffix_lengths, ready, fresh, suffix_keys, suffix_values)
    packet, sums, maxima, totals = lax.optimization_barrier((packet, sums, maxima, totals))
    parts = exchange(packet, "ctx")
    attention = merge_copies(parts, sums, maxima, totals, group, rows // n_ctx)
    attention = exchange(attention, "ctx")
    pieces = send_pieces(project_out(attention, out_weight), "head")
    result = pieces[0].astype(F32)
    for piece in pieces[1:]:
        result = result + piece.astype(F32)
    return result.astype(BF16).reshape(batch // n_head, steps, -1)


def solution(mesh):
    placed = (
        P(),
        P(),
        P("ctx", "head"),
        P("head"),
        P("head", None, "ctx"),
        P("head", "ctx"),
        P("head", "ctx", None),
        P("head", "ctx", None),
        P("ctx", None, "head", None),
        P("ctx", None, "head", None),
    )
    return jax.shard_map(
        body, mesh=mesh, in_specs=placed, out_specs=P("head", None, "ctx"), check_vma=False
    )
```

```python
import functools

import jax
import jax.numpy as jnp
import numpy as np
from jax import lax
from jax.experimental import pallas as pl
from jax.experimental.pallas import tpu as pltpu
from jax.sharding import PartitionSpec as P

EPSILON = 1e-05
ROTARY_THETA = 500000.0
MASKED = -1e30
BF16 = jnp.bfloat16
F32 = jnp.float32
LANES = 128
MIB = 1 << 20
VMEM = pl.BlockSpec(memory_space=pltpu.VMEM)
SMEM = pl.BlockSpec(memory_space=pltpu.SMEM)
HBM = pl.BlockSpec(memory_space=pl.ANY)
NT = (((1,), (1,)), ((), ()))


def round_up(value, unit):
    return -(-value // unit) * unit


def params(limit):
    return pltpu.CompilerParams(vmem_limit_bytes=min(limit, 60 * MIB))


def cost(flops, moved, transcendentals=0):
    return pl.CostEstimate(flops=flops, bytes_accessed=moved, transcendentals=transcendentals)


def exchange(blocks, axis):
    return lax.all_to_all(blocks, axis, 0, 0)


def send_pieces(pieces, axis):
    count = lax.axis_size(axis)
    received = [pieces[0]]
    for shift in range(1, count):
        pairs = [(i, (i + shift) % count) for i in range(count)]
        received.append(lax.ppermute(pieces[shift], axis, pairs))
    return received


def token_at(tokens, row):
    steps = tokens.shape[0]
    return tokens[row % steps, row // steps]


def assign_slots(tokens, rows, owners, local_rows, capacity):
    lanes = round_up(rows, LANES)
    down = lax.broadcasted_iota(jnp.int32, (rows, lanes), 0)
    across = lax.broadcasted_iota(jnp.int32, (rows, lanes), 1)
    column = jnp.zeros((rows, lanes), jnp.int32)
    line = jnp.full((rows, lanes), -1, jnp.int32)
    for row in range(rows):
        token = token_at(tokens, row)
        column = jnp.where(down == row, token, column)
        line = jnp.where(across == row, token, line)
    owner_column = jnp.zeros((rows, lanes), F32)
    owner_line = jnp.zeros((rows, lanes), F32)
    for owner in range(1, owners):
        owner_column += jnp.where(column >= owner * local_rows, 1.0, 0.0)
        owner_line += jnp.where(line >= owner * local_rows, 1.0, 0.0)
    same = jnp.where(column == line, 1.0, 0.0)
    index = across.astype(F32)
    earliest = jnp.min(jnp.where(same > 0, index, float(lanes)), axis=1, keepdims=True)
    repeated = jnp.max(jnp.where(down < across, same, 0.0), axis=0, keepdims=True)
    counted = jnp.where((repeated == 0) & (across < rows) & (index < earliest), 1.0, 0.0)
    slot = jnp.sum(jnp.where(owner_column == owner_line, counted, 0.0), axis=1, keepdims=True)
    place = jnp.where(slot < capacity, owner_column[:, :1] * capacity + slot, -1.0)
    first = earliest == down[:, :1].astype(F32)
    return place, first


def rotary_tables(lengths, steps, rows, context, head_dim):
    half = head_dim // 2
    down = lax.broadcasted_iota(jnp.int32, (rows, head_dim), 0)
    across = lax.broadcasted_iota(jnp.int32, (1, head_dim), 1)
    frequency = jnp.zeros((1, head_dim), F32)
    for i in range(half):
        value = float(np.float32(ROTARY_THETA ** (-2.0 * i / head_dim)))
        frequency = jnp.where(across % half == i, value, frequency)
    length = jnp.zeros((rows, head_dim), jnp.int32)
    for sequence in range(rows // steps):
        length = jnp.where(down // steps == sequence, lengths[sequence], length)
    positions = (context + length + down % steps).astype(F32)
    angles = positions * frequency
    sine = jnp.sin(angles)
    return jnp.cos(angles), jnp.where(across < half, -sine, sine)


def tables_kernel(steps, context, lengths, cosine, sine):
    rows, head_dim = cosine.shape
    cosine[...], sine[...] = rotary_tables(lengths, steps, rows, context, head_dim)


def tables(lengths, steps, rows, context, head_dim):
    return pl.pallas_call(
        functools.partial(tables_kernel, steps, context),
        out_shape=[jax.ShapeDtypeStruct((rows, head_dim), F32)] * 2,
        in_specs=[SMEM],
        out_specs=[VMEM] * 2,
        compiler_params=params(8 * MIB),
        name="tables",
    )(lengths)


def fetch_rows(tokens, table, blocks, rows_f32, sem, between=None):
    rows = rows_f32.shape[0]
    local_rows = table.shape[0]
    base = lax.axis_index("ctx") * local_rows

    def find(row):
        offset = token_at(tokens, row) - base
        return offset, (offset >= 0) & (offset < local_rows)

    def copy(row, offset):
        start = pl.multiple_of((offset // 8) * 8, 8)
        return pltpu.make_async_copy(
            table.at[pl.ds(start, 8), :], blocks.at[row], sem.at[row]
        )

    for row in range(rows):
        offset, inside = find(row)

        @pl.when(inside)
        def _():
            copy(row, offset).start()

    rows_f32[...] = jnp.zeros_like(rows_f32)
    result = None if between is None else between()
    sublane = lax.broadcasted_iota(jnp.int32, (8, 1), 0)
    for row in range(rows):
        offset, inside = find(row)

        @pl.when(inside)
        def _():
            copy(row, offset).wait()
            picked = jnp.where(sublane == offset % 8, blocks[row].astype(F32), 0.0)
            rows_f32[row : row + 1, :] = jnp.sum(picked, axis=0, keepdims=True)

    return result


def lookup_kernel(
    owners, context, tokens, lengths, table, packed, places, crowded, cosine, sine, blocks, rows_f32, sem
):
    capacity, _ = packed.shape
    rows, head_dim = cosine.shape

    def between():
        cosine[...], sine[...] = rotary_tables(lengths, tokens.shape[0], rows, context, head_dim)
        return assign_slots(tokens, rows, owners, table.shape[0], capacity)

    place, first = fetch_rows(tokens, table, blocks, rows_f32, sem, between)
    places[...] = jnp.broadcast_to(place, places.shape)
    crowded[0] = jnp.max(jnp.where(place < 0, 1, 0))
    slot = lax.broadcasted_iota(jnp.int32, (rows, capacity), 1) + lax.axis_index("ctx") * capacity
    chosen = jnp.where((place == slot.astype(F32)) & first, 1.0, 0.0).astype(BF16)
    packed[...] = lax.dot_general(
        chosen, rows_f32[...].astype(BF16), (((0,), (0,)), ((), ())), preferred_element_type=F32
    ).astype(BF16)


def rest_kernel(tokens, places, table, out, blocks, rows_f32, sem):
    chunks, rows, width = out.shape
    fetch_rows(tokens, table, blocks, rows_f32, sem)
    left = places[...][:, :1] < 0
    for chunk in range(chunks):
        found = rows_f32[:, chunk * width : (chunk + 1) * width]
        out[chunk] = jnp.where(left, found, 0.0).astype(BF16)


def fetch_scratch(rows, width):
    return [
        pltpu.VMEM((rows, 8, width), BF16),
        pltpu.VMEM((rows, width), F32),
        pltpu.SemaphoreType.DMA((rows,)),
    ]


def spread_kernel(block, first, out):
    for target in range(out.shape[0]):
        out[target] = block[...]


def spread(block, first, hint):
    count = lax.axis_size("ctx")
    return pl.pallas_call(
        spread_kernel,
        out_shape=jax.ShapeDtypeStruct((count,) + block.shape, block.dtype),
        in_specs=[VMEM, HBM],
        out_specs=VMEM,
        compiler_params=params(8 * MIB),
        cost_estimate=cost(400 * hint, hint),
        name="spread",
    )(block, first)


def lookup_packed(token_ids, lengths, embedding, capacity, context, head_dim):
    steps, batch = token_ids.shape
    rows = steps * batch
    owners = lax.axis_size("ctx")
    _, width = embedding.shape
    return pl.pallas_call(
        functools.partial(lookup_kernel, owners, context),
        out_shape=[
            jax.ShapeDtypeStruct((capacity, width), BF16),
            jax.ShapeDtypeStruct((rows, LANES), F32),
            jax.ShapeDtypeStruct((1,), jnp.int32),
            jax.ShapeDtypeStruct((rows, head_dim), F32),
            jax.ShapeDtypeStruct((rows, head_dim), F32),
        ],
        in_specs=[SMEM, SMEM, HBM],
        out_specs=[VMEM, VMEM, SMEM, VMEM, VMEM],
        scratch_shapes=fetch_scratch(rows, width),
        compiler_params=params(6 * rows * width * 8),
        cost_estimate=cost(rows * width, rows * width * 16),
        name="lookup",
    )(token_ids, lengths, embedding)


def lookup_rest(token_ids, places, embedding):
    rows = places.shape[0]
    chunks = lax.axis_size("ctx")
    _, width = embedding.shape
    return pl.pallas_call(
        rest_kernel,
        out_shape=jax.ShapeDtypeStruct((chunks, rows, width // chunks), BF16),
        in_specs=[SMEM, VMEM, HBM],
        out_specs=VMEM,
        scratch_shapes=fetch_scratch(rows, width),
        compiler_params=params(6 * rows * width * 8),
        name="rest",
    )(token_ids, places, embedding)


def lookup_all(token_ids, embedding):
    steps, batch = token_ids.shape
    rows = steps * batch
    chunks = lax.axis_size("ctx")
    local_rows, width = embedding.shape
    offsets = token_ids.T.reshape(rows) - lax.axis_index("ctx") * local_rows
    inside = (offsets >= 0) & (offsets < local_rows)
    picked = jnp.take(embedding, jnp.clip(offsets, 0, local_rows - 1), axis=0)
    picked = jnp.where(inside[:, None], picked, jnp.zeros((), BF16))
    return jnp.swapaxes(picked.reshape(rows, chunks, width // chunks), 0, 1)


def join_kernel(parts, out):
    total = parts[0].astype(F32)
    for source in range(1, parts.shape[0]):
        total = total + parts[source].astype(F32)
    joined = total.astype(BF16)
    for target in range(out.shape[0]):
        out[target] = joined


def join_copies(parts):
    return pl.pallas_call(
        join_kernel,
        out_shape=jax.ShapeDtypeStruct(parts.shape, BF16),
        in_specs=[VMEM],
        out_specs=VMEM,
        compiler_params=params(8 * MIB),
        name="join",
    )(parts)


def project_kernel(heads_here, packed, x, gain, weight, *refs):
    if packed:
        slots, places, *refs = refs
    count = weight.shape[0] // heads_here
    outs, scaled = refs[:count], refs[count]
    chunks, rows, chunk_width = x.shape
    if packed:
        owners, capacity, width = slots.shape
        held = slots[...].astype(F32).reshape(owners * capacity, width).astype(BF16)
        slot = lax.broadcasted_iota(jnp.int32, (rows, owners * capacity), 1).astype(F32)
        chosen = jnp.where(places[...][:, :1] == slot, 1.0, 0.0).astype(BF16)
    columns = weight.shape[1]
    here = lax.axis_index("head")
    squares = jnp.zeros((rows, 1), F32)
    for chunk in range(chunks):
        span = slice(chunk * chunk_width, (chunk + 1) * chunk_width)
        features = x[chunk].astype(F32)
        if packed:
            features += jnp.dot(chosen, held[:, span], preferred_element_type=F32)
        squares = squares + jnp.sum(features * features, axis=-1, keepdims=True)
        scaled[:, span] = (features * gain[:, span]).astype(BF16)
    used = heads_here * columns
    rest = outs[0].shape[1] - used
    for shift in range(count):
        first = lax.rem(here + shift, count) * heads_here
        products = [
            lax.dot_general(scaled[...], weight[first + head], NT, preferred_element_type=F32)
            for head in range(heads_here)
        ]
        outs[shift][...] = jnp.concatenate(
            products + [jnp.broadcast_to(squares, (rows, rest))], axis=1
        )


def project(x, attn_gain, weight, packed=()):
    count = lax.axis_size("head")
    chunks, rows, chunk_width = x.shape
    heads, columns, width = weight.shape
    heads_here = heads // count
    wide = round_up(heads_here * columns + 1, LANES)
    size = weight.size * 2
    return pl.pallas_call(
        functools.partial(project_kernel, heads_here, bool(packed)),
        out_shape=[jax.ShapeDtypeStruct((rows, wide), F32)] * count,
        in_specs=[VMEM] * (3 + len(packed)),
        out_specs=[VMEM] * count,
        scratch_shapes=[pltpu.VMEM((rows, width), BF16)],
        compiler_params=params(8 * MIB),
        cost_estimate=cost(2 * rows * weight.size, size),
        name="project",
    )(x, attn_gain.reshape(1, width), weight, *packed)


def norm_kernel(used, model_width, *refs):
    pieces, out = refs[:-1], refs[-1]
    total = pieces[0][...]
    for piece in pieces[1:]:
        total = total + piece[...]
    factor = lax.rsqrt(total[:, used : used + 1] * (1.0 / model_width) + EPSILON)
    united = (total * factor).astype(BF16)
    for target in range(out.shape[0]):
        out[target] = united


def norm_copies(pieces, used, model_width):
    rows, wide = pieces[0].shape
    return pl.pallas_call(
        functools.partial(norm_kernel, used, model_width),
        out_shape=jax.ShapeDtypeStruct((lax.axis_size("ctx"), rows, wide), BF16),
        in_specs=[VMEM] * len(pieces),
        out_specs=VMEM,
        compiler_params=params(8 * MIB),
        name="norm",
    )(*pieces)


def split3(value):
    first = value.astype(BF16).astype(F32)
    second = (value - first).astype(BF16).astype(F32)
    return first, second, value - first - second


def near_block(query, fresh_key, fresh_value, keys, values, head, heads, steps, lengths):
    owned, slots_all, _ = keys.shape
    block = query.shape[0]
    rows = fresh_key.shape[0]
    mine = lax.axis_index("ctx")

    def iota(shape, axis):
        return lax.broadcasted_iota(jnp.int32, shape, axis)

    query_place = iota((block, 1), 0) % (owned * steps)
    sequence = query_place // steps
    step = query_place % steps
    slot = iota((1, slots_all), 1)
    fresh_row = iota((1, rows), 1)
    fresh_here = (fresh_row // steps == mine * owned + sequence) & (fresh_row % steps <= step)
    fresh_scores = lax.dot_general(query, fresh_key, NT, preferred_element_type=F32)
    scores = [jnp.where(fresh_here, fresh_scores, MASKED)]
    highest = jnp.max(scores[0], axis=-1, keepdims=True)
    for s in range(owned):
        found = lax.dot_general(query, keys[s], NT, preferred_element_type=F32)
        live = (sequence == s) & (slot % heads == head)
        live = live & (slot // heads < lengths[mine * owned + s])
        found = jnp.where(live, found, MASKED)
        scores.append(found)
        highest = jnp.maximum(highest, jnp.max(found, axis=-1, keepdims=True))
    total = jnp.zeros((block, 1), F32)
    result = jnp.zeros((block, fresh_value.shape[1]), F32)
    for found, value in zip(scores, [fresh_value] + [values[s] for s in range(owned)]):
        weights = jnp.exp(found - highest).astype(BF16)
        total = total + jnp.sum(weights.astype(F32), axis=-1, keepdims=True)
        result = result + jnp.dot(weights, value, preferred_element_type=F32)
    return highest, total, result


def attend_kernel(
    columns,
    group,
    owned,
    lengths,
    united,
    cosine,
    sine,
    keys,
    values,
    slot_keys,
    slot_values,
    packet,
    near_sums,
    near_maxima,
    near_totals,
    query_buf,
    score_buf,
):
    chunks, rows, _ = united.shape
    heads, context, head_dim = keys.shape
    per_dest = rows // chunks
    block = per_dest * group
    tile = min(512, context)
    tiles = context // tile
    cos = cosine[...]
    sin = sine[...]
    mine = lax.axis_index("ctx")

    def rotated(vectors):
        return vectors * cos + pltpu.roll(vectors, head_dim // 2, 1) * sin

    fresh = []
    for head in range(heads):
        first = head * columns
        whole = jnp.concatenate(
            [united[chunk].astype(F32)[:, first : first + columns] for chunk in range(chunks)],
            axis=1,
        )
        for j in range(group):
            query = rotated(whole[:, j * head_dim : (j + 1) * head_dim]) * head_dim ** (-0.5)
            for dest in range(chunks):
                start = dest * block + j * per_dest
                query_buf[head, start : start + per_dest, :] = query[
                    dest * per_dest : (dest + 1) * per_dest
                ]
        new_key = rotated(whole[:, group * head_dim : (group + 1) * head_dim])
        new_value = whole[:, (group + 1) * head_dim :]
        fresh.append((new_key.astype(BF16), new_value.astype(BF16)))

    lane = lax.broadcasted_iota(jnp.int32, (chunks * block, LANES), 1)
    table = jnp.zeros((chunks * block, LANES), F32)
    for head in range(heads):
        query = query_buf[head].astype(BF16)
        highest = None
        for step in range(tiles):
            span = slice(step * tile, (step + 1) * tile)
            scores = lax.dot_general(
                query, keys[head, span, :], NT, preferred_element_type=F32
            )
            score_buf[:, span] = scores
            for part in range(tile // LANES):
                piece = scores[:, part * LANES : (part + 1) * LANES]
                highest = piece if highest is None else jnp.maximum(highest, piece)
        maxima = jnp.max(highest, axis=-1, keepdims=True)
        sums = jnp.zeros((chunks * block, head_dim), F32)
        totals = jnp.zeros((chunks * block, LANES), F32)
        for step in range(tiles):
            span = slice(step * tile, (step + 1) * tile)
            weights = jnp.exp(score_buf[:, span] - maxima).astype(BF16)
            sums = sums + jnp.dot(weights, values[head, span, :], preferred_element_type=F32)
            wide = weights.astype(F32)
            for part in range(tile // LANES):
                totals = totals + wide[:, part * LANES : (part + 1) * LANES]
        total = jnp.sum(totals, axis=-1, keepdims=True)
        for index, piece in enumerate(split3(maxima) + split3(total)):
            table = jnp.where(lane == head * 8 + index, piece, table)
        rounded = sums.astype(BF16)
        for dest in range(chunks):
            packet[dest, head * block : (head + 1) * block] = rounded[
                dest * block : (dest + 1) * block
            ]
        own_query = query_buf[head, pl.ds(pl.multiple_of(mine * block, block), block), :]
        near_max, near_total, near_sum = near_block(
            own_query.astype(BF16),
            *fresh[head],
            slot_keys,
            slot_values,
            head,
            heads,
            per_dest // owned,
            lengths,
        )
        span = slice(head * block, (head + 1) * block)
        near_sums[span, :] = near_sum
        near_maxima[span, :] = jnp.broadcast_to(near_max, (block, head_dim))
        near_totals[span, :] = jnp.broadcast_to(near_total, (block, head_dim))
    low = heads * block
    pieces = packet.shape[1] - low
    turned = jnp.transpose(table)[:pieces]
    for dest in range(chunks):
        packet[dest, low:, :block] = turned[:, dest * block : (dest + 1) * block].astype(BF16)


def attend(united, columns, cosine, sine, keys, values, lengths, slot_keys, slot_values):
    chunks, rows, _ = united.shape
    heads, context, head_dim = keys.shape
    owned, slots, _, _ = slot_keys.shape
    group = columns * chunks // head_dim - 2
    block = rows // chunks * group
    size = keys.size * 2
    flat = chunks * block
    near = jax.ShapeDtypeStruct((heads * block, head_dim), F32)
    return pl.pallas_call(
        functools.partial(attend_kernel, columns, group, owned),
        out_shape=[
            jax.ShapeDtypeStruct((chunks, heads * block + round_up(heads * 8, 16), head_dim), BF16),
            near,
            near,
            near,
        ],
        in_specs=[SMEM] + [VMEM] * 7,
        out_specs=[VMEM] * 4,
        scratch_shapes=[
            pltpu.VMEM((heads, flat, head_dim), F32),
            pltpu.VMEM((flat, context), F32),
        ],
        compiler_params=params(flat * context * 4 + 12 * MIB),
        cost_estimate=cost(4 * heads * flat * context * head_dim, 2 * size, heads * flat * context),
        name="attend",
    )(
        lengths,
        united,
        cosine,
        sine,
        keys,
        values,
        slot_keys.reshape(owned, slots * heads, head_dim),
        slot_values.reshape(owned, slots * heads, head_dim),
    )


def merge_kernel(group, parts, near_sums, near_maxima, near_totals, out, places, stats):
    chunks = parts.shape[0]
    per_dest = out.shape[1]
    block = per_dest * group
    queries, head_dim = near_sums.shape
    heads = queries // block
    highest = near_maxima[...][:, :1]
    maxima, totals = [], []
    pieces = parts.shape[1] - queries
    for source in range(chunks):
        stats[source * pieces : (source + 1) * pieces, :] = parts[source, queries:, :].astype(F32)
    turned = jnp.transpose(stats[...])[:block]
    for source in range(chunks):
        m, t = [], []
        for head in range(heads):
            column = source * pieces + head * 8
            get = lambda k: turned[:, column + k : column + k + 1]
            m.append(get(0) + get(1) + get(2))
            t.append(get(3) + get(4) + get(5))
        maxima.append(jnp.concatenate(m, axis=0))
        totals.append(jnp.concatenate(t, axis=0))
        highest = jnp.maximum(highest, maxima[-1])
    scale = jnp.exp(near_maxima[...][:, :1] - highest)
    numerator = near_sums[...] * scale
    denominator = near_totals[...][:, :1] * scale
    for source in range(chunks):
        scale = jnp.exp(maxima[source] - highest)
        numerator = numerator + parts[source, :queries, :].astype(F32) * scale
        denominator = denominator + totals[source] * scale
    attention = numerator / denominator
    for index in range(heads * group):
        places[:, index * head_dim : (index + 1) * head_dim] = attention[
            index * per_dest : (index + 1) * per_dest
        ]
    rounded = places[...].astype(BF16)
    for target in range(chunks):
        out[target] = rounded


def merge_copies(parts, sums, maxima, totals, group, per_dest):
    chunks = parts.shape[0]
    queries, head_dim = sums.shape
    heads = queries // (per_dest * group)
    width = heads * group * head_dim
    return pl.pallas_call(
        functools.partial(merge_kernel, group),
        out_shape=jax.ShapeDtypeStruct((chunks, per_dest, width), BF16),
        in_specs=[VMEM] * 4,
        out_specs=VMEM,
        scratch_shapes=[
            pltpu.VMEM((per_dest, width), F32),
            pltpu.VMEM((chunks * (parts.shape[1] - queries), head_dim), F32),
        ],
        compiler_params=params(12 * MIB),
        name="merge",
    )(parts, sums, maxima, totals)


def output_kernel(x, weight, *refs):
    chunks, per_dest, depth = x.shape
    rows_f32, total = refs[-2:]
    outs = refs[:-2]
    count = len(outs)
    for chunk in range(chunks):
        rows_f32[chunk * per_dest : (chunk + 1) * per_dest, :] = x[chunk].astype(F32)
    total[...] = jnp.dot(
        rows_f32[...].astype(BF16), weight[...], preferred_element_type=F32
    )
    here = lax.axis_index("head")
    height = total.shape[0] // count
    for shift in range(count):
        first = pl.multiple_of(lax.rem(here + shift, count) * height, height)
        outs[shift][...] = total[pl.ds(first, height), :].astype(BF16)


def project_out(x, weight):
    count = lax.axis_size("head")
    chunks, per_dest, depth = x.shape
    rows = chunks * per_dest
    width = weight.shape[1]
    return pl.pallas_call(
        output_kernel,
        out_shape=[jax.ShapeDtypeStruct((rows // count, width), BF16)] * count,
        in_specs=[VMEM, VMEM],
        out_specs=[VMEM] * count,
        scratch_shapes=[pltpu.VMEM((rows, depth), F32), pltpu.VMEM((rows, width), F32)],
        compiler_params=params(8 * MIB),
        cost_estimate=cost(2 * rows * weight.size, weight.size * 2),
        name="output",
    )(x, weight)


def body(
    token_ids,
    suffix_lengths,
    embedding,
    attn_gain,
    qkv_weight,
    out_weight,
    prefix_keys,
    prefix_values,
    suffix_keys,
    suffix_values,
):
    steps, batch = token_ids.shape
    rows = steps * batch
    n_ctx = lax.axis_size("ctx")
    n_head = lax.axis_size("head")
    heads, block_context, head_dim = prefix_keys.shape
    width = embedding.shape[1]
    columns = qkv_weight.shape[2]
    group = columns * n_ctx // head_dim - 2
    context = block_context * n_ctx
    capacity = 2 * rows // n_ctx
    qkv_weight = jnp.transpose(qkv_weight, (1, 2, 0))
    if embedding.shape[0] % 8 == 0 and capacity % 8 == 0:
        packed, places, crowded, cosine, sine = lookup_packed(
            token_ids, suffix_lengths, embedding, capacity, context, head_dim
        )

        def rest():
            found = lookup_rest(token_ids, places, embedding)
            return exchange(join_copies(exchange(found, "ctx")), "ctx")

        def nothing():
            return jnp.zeros((n_ctx, rows, width // n_ctx), BF16)

        features = lax.cond(crowded[0] > 0, rest, nothing)
        packed = exchange(spread(packed, features, 4 * qkv_weight.size), "ctx")
        pieces = project(features, attn_gain, qkv_weight, (packed, places))
    else:
        cosine, sine = tables(suffix_lengths, steps, rows, context, head_dim)
        joined = join_copies(exchange(lookup_all(token_ids, embedding), "ctx"))
        pieces = project(exchange(joined, "ctx"), attn_gain, qkv_weight)
    pieces = send_pieces(pieces, "head")
    united = norm_copies(pieces, heads * columns, width * n_head)
    united = exchange(united, "ctx")
    packet, sums, maxima, totals = attend(
        united,
        columns,
        cosine,
        sine,
        prefix_keys,
        prefix_values,
        suffix_lengths,
        suffix_keys,
        suffix_values,
    )
    parts = exchange(packet, "ctx")
    attention = merge_copies(parts, sums, maxima, totals, group, rows // n_ctx)
    attention = exchange(attention, "ctx")
    pieces = send_pieces(project_out(attention, out_weight), "head")
    result = pieces[0].astype(F32)
    for piece in pieces[1:]:
        result = result + piece.astype(F32)
    return result.astype(BF16).reshape(batch // n_head, steps, -1)


def solution(mesh):
    placed = (
        P(),
        P(),
        P("ctx", "head"),
        P("head"),
        P("head", None, "ctx"),
        P("head", "ctx"),
        P("head", "ctx", None),
        P("head", "ctx", None),
        P("ctx", None, "head", None),
        P("ctx", None, "head", None),
    )
    return jax.shard_map(
        body, mesh=mesh, in_specs=placed, out_specs=P("head", None, "ctx"), check_vma=False
    )
```

```python
import functools

import jax
import jax.numpy as jnp
import numpy as np
from jax import lax
from jax.experimental import pallas as pl
from jax.experimental.pallas import tpu as pltpu
from jax.sharding import PartitionSpec as P

EPSILON = 1e-05
ROTARY_THETA = 500000.0
MASKED = -1e30
BF16 = jnp.bfloat16
F32 = jnp.float32
LANES = 128
MIB = 1 << 20
VMEM = pl.BlockSpec(memory_space=pltpu.VMEM)
SMEM = pl.BlockSpec(memory_space=pltpu.SMEM)
HBM = pl.BlockSpec(memory_space=pl.ANY)
NT = (((1,), (1,)), ((), ()))


def round_up(value, unit):
    return -(-value // unit) * unit


def params(limit):
    return pltpu.CompilerParams(vmem_limit_bytes=min(limit, 60 * MIB))


def cost(flops, moved, transcendentals=0):
    return pl.CostEstimate(flops=flops, bytes_accessed=moved, transcendentals=transcendentals)


def exchange(blocks, axis):
    return lax.all_to_all(blocks, axis, 0, 0)


def partner(here, shift, count):
    if count & (count - 1) == 0:
        return here ^ shift
    return (here + shift) % count


def send_pieces(pieces, axis):
    count = lax.axis_size(axis)
    received = [pieces[0]]
    for shift in range(1, count):
        pairs = [(i, partner(i, shift, count)) for i in range(count)]
        received.append(lax.ppermute(pieces[shift], axis, pairs))
    return received


def token_at(tokens, row):
    steps = tokens.shape[0]
    return tokens[row % steps, row // steps]


def assign_slots(tokens, rows, owners, local_rows, capacity):
    lanes = round_up(rows, LANES)
    down = lax.broadcasted_iota(jnp.int32, (rows, lanes), 0)
    across = lax.broadcasted_iota(jnp.int32, (rows, lanes), 1)
    column = jnp.zeros((rows, lanes), jnp.int32)
    line = jnp.full((rows, lanes), -1, jnp.int32)
    for row in range(rows):
        token = token_at(tokens, row)
        column = jnp.where(down == row, token, column)
        line = jnp.where(across == row, token, line)
    owner_column = jnp.zeros((rows, lanes), F32)
    owner_line = jnp.zeros((rows, lanes), F32)
    for owner in range(1, owners):
        owner_column += jnp.where(column >= owner * local_rows, 1.0, 0.0)
        owner_line += jnp.where(line >= owner * local_rows, 1.0, 0.0)
    same = jnp.where(column == line, 1.0, 0.0)
    index = across.astype(F32)
    earliest = jnp.min(jnp.where(same > 0, index, float(lanes)), axis=1, keepdims=True)
    repeated = jnp.max(jnp.where(down < across, same, 0.0), axis=0, keepdims=True)
    counted = jnp.where((repeated == 0) & (across < rows) & (index < earliest), 1.0, 0.0)
    slot = jnp.sum(jnp.where(owner_column == owner_line, counted, 0.0), axis=1, keepdims=True)
    place = jnp.where(slot < capacity, owner_column[:, :1] * capacity + slot, -1.0)
    first = earliest == down[:, :1].astype(F32)
    return place, first


def rotary_tables(lengths, steps, rows, context, head_dim):
    half = head_dim // 2
    down = lax.broadcasted_iota(jnp.int32, (rows, head_dim), 0)
    across = lax.broadcasted_iota(jnp.int32, (1, head_dim), 1)
    frequency = jnp.zeros((1, head_dim), F32)
    for i in range(half):
        value = float(np.float32(ROTARY_THETA ** (-2.0 * i / head_dim)))
        frequency = jnp.where(across % half == i, value, frequency)
    length = jnp.zeros((rows, head_dim), jnp.int32)
    for sequence in range(rows // steps):
        length = jnp.where(down // steps == sequence, lengths[sequence], length)
    positions = (context + length + down % steps).astype(F32)
    angles = positions * frequency
    sine = jnp.sin(angles)
    return jnp.cos(angles), jnp.where(across < half, -sine, sine)


def fetch_rows(tokens, table, blocks, rows_f32, sem, between=None):
    rows = rows_f32.shape[0]
    local_rows = table.shape[0]
    base = lax.axis_index("ctx") * local_rows

    def find(row):
        offset = token_at(tokens, row) - base
        return offset, (offset >= 0) & (offset < local_rows)

    def copy(row, offset):
        start = pl.multiple_of((offset // 8) * 8, 8)
        return pltpu.make_async_copy(
            table.at[pl.ds(start, 8), :], blocks.at[row], sem.at[row]
        )

    for row in range(rows):
        offset, inside = find(row)

        @pl.when(inside)
        def _():
            copy(row, offset).start()

    rows_f32[...] = jnp.zeros_like(rows_f32)
    result = None if between is None else between()
    sublane = lax.broadcasted_iota(jnp.int32, (8, 1), 0)
    for row in range(rows):
        offset, inside = find(row)

        @pl.when(inside)
        def _():
            copy(row, offset).wait()
            picked = jnp.where(sublane == offset % 8, blocks[row].astype(F32), 0.0)
            rows_f32[row : row + 1, :] = jnp.sum(picked, axis=0, keepdims=True)

    return result


def lookup_kernel(
    owners, tokens, table, packed, places, crowded, blocks, rows_f32, sem
):
    capacity, _ = packed.shape
    rows = rows_f32.shape[0]

    def between():
        return assign_slots(tokens, rows, owners, table.shape[0], capacity)

    place, first = fetch_rows(tokens, table, blocks, rows_f32, sem, between)
    places[...] = jnp.broadcast_to(place, places.shape)
    crowded[0] = jnp.max(jnp.where(place < 0, 1, 0))
    slot = lax.broadcasted_iota(jnp.int32, (rows, capacity), 1) + lax.axis_index("ctx") * capacity
    chosen = jnp.where((place == slot.astype(F32)) & first, 1.0, 0.0).astype(BF16)
    packed[...] = lax.dot_general(
        chosen, rows_f32[...].astype(BF16), (((0,), (0,)), ((), ())), preferred_element_type=F32
    ).astype(BF16)


def rest_kernel(tokens, places, table, out, blocks, rows_f32, sem):
    chunks, rows, width = out.shape
    fetch_rows(tokens, table, blocks, rows_f32, sem)
    left = places[...][:, :1] < 0
    for chunk in range(chunks):
        found = rows_f32[:, chunk * width : (chunk + 1) * width]
        out[chunk] = jnp.where(left, found, 0.0).astype(BF16)


def fetch_scratch(rows, width):
    return [
        pltpu.VMEM((rows, 8, width), BF16),
        pltpu.VMEM((rows, width), F32),
        pltpu.SemaphoreType.DMA((rows,)),
    ]


def spread_kernel(block, first, out):
    for target in range(out.shape[0]):
        out[target] = block[...]


def spread(block, first, hint):
    count = lax.axis_size("ctx")
    return pl.pallas_call(
        spread_kernel,
        out_shape=jax.ShapeDtypeStruct((count,) + block.shape, block.dtype),
        in_specs=[VMEM, HBM],
        out_specs=VMEM,
        compiler_params=params(8 * MIB),
        cost_estimate=cost(400 * hint, hint),
        name="spread",
    )(block, first)


def lookup_packed(token_ids, embedding, capacity):
    steps, batch = token_ids.shape
    rows = steps * batch
    owners = lax.axis_size("ctx")
    _, width = embedding.shape
    return pl.pallas_call(
        functools.partial(lookup_kernel, owners),
        out_shape=[
            jax.ShapeDtypeStruct((capacity, width), BF16),
            jax.ShapeDtypeStruct((rows, LANES), F32),
            jax.ShapeDtypeStruct((1,), jnp.int32),
        ],
        in_specs=[SMEM, HBM],
        out_specs=[VMEM, VMEM, SMEM],
        scratch_shapes=fetch_scratch(rows, width),
        compiler_params=params(6 * rows * width * 8),
        cost_estimate=cost(rows * width, rows * width * 16),
        name="lookup",
    )(token_ids, embedding)


def lookup_rest(token_ids, places, embedding):
    rows = places.shape[0]
    chunks = lax.axis_size("ctx")
    _, width = embedding.shape
    return pl.pallas_call(
        rest_kernel,
        out_shape=jax.ShapeDtypeStruct((chunks, rows, width // chunks), BF16),
        in_specs=[SMEM, VMEM, HBM],
        out_specs=VMEM,
        scratch_shapes=fetch_scratch(rows, width),
        compiler_params=params(6 * rows * width * 8),
        name="rest",
    )(token_ids, places, embedding)


def lookup_all(token_ids, embedding):
    steps, batch = token_ids.shape
    rows = steps * batch
    chunks = lax.axis_size("ctx")
    local_rows, width = embedding.shape
    offsets = token_ids.T.reshape(rows) - lax.axis_index("ctx") * local_rows
    inside = (offsets >= 0) & (offsets < local_rows)
    picked = jnp.take(embedding, jnp.clip(offsets, 0, local_rows - 1), axis=0)
    picked = jnp.where(inside[:, None], picked, jnp.zeros((), BF16))
    return jnp.swapaxes(picked.reshape(rows, chunks, width // chunks), 0, 1)


def join_kernel(parts, out):
    total = parts[0].astype(F32)
    for source in range(1, parts.shape[0]):
        total = total + parts[source].astype(F32)
    joined = total.astype(BF16)
    for target in range(out.shape[0]):
        out[target] = joined


def join_copies(parts):
    return pl.pallas_call(
        join_kernel,
        out_shape=jax.ShapeDtypeStruct(parts.shape, BF16),
        in_specs=[VMEM],
        out_specs=VMEM,
        compiler_params=params(8 * MIB),
        name="join",
    )(parts)


def project_kernel(heads_here, packed, steps, context, x, gain, weight, lengths, *refs):
    if packed:
        slots, places, *refs = refs
    count = weight.shape[0] // heads_here
    outs, (cosine, sine, scaled) = refs[:count], refs[count:]
    chunks, rows, chunk_width = x.shape
    if packed:
        owners, capacity, width = slots.shape
        held = slots[...].astype(F32).reshape(owners * capacity, width).astype(BF16)
        slot = lax.broadcasted_iota(jnp.int32, (rows, owners * capacity), 1).astype(F32)
        chosen = jnp.where(places[...][:, :1] == slot, 1.0, 0.0).astype(BF16)
    columns = weight.shape[1]
    here = lax.axis_index("head")
    squares = jnp.zeros((rows, 1), F32)
    for chunk in range(chunks):
        span = slice(chunk * chunk_width, (chunk + 1) * chunk_width)
        features = x[chunk].astype(F32)
        if packed:
            features += jnp.dot(chosen, held[:, span], preferred_element_type=F32)
        squares = squares + jnp.sum(features * features, axis=-1, keepdims=True)
        scaled[:, span] = (features * gain[:, span]).astype(BF16)
    used = heads_here * columns
    rest = outs[0].shape[1] - used
    for shift in range(count):
        first = partner(here, shift, count) * heads_here
        products = [
            lax.dot_general(scaled[...], weight[first + head], NT, preferred_element_type=F32)
            for head in range(heads_here)
        ]
        outs[shift][...] = jnp.concatenate(
            products + [jnp.broadcast_to(squares, (rows, rest))], axis=1
        )
    cosine[...], sine[...] = rotary_tables(lengths, steps, rows, context, cosine.shape[1])


def project(x, attn_gain, weight, lengths, steps, context, head_dim, packed):
    count = lax.axis_size("head")
    chunks, rows, chunk_width = x.shape
    heads, columns, width = weight.shape
    heads_here = heads // count
    wide = round_up(heads_here * columns + 1, LANES)
    size = weight.size * 2
    return pl.pallas_call(
        functools.partial(project_kernel, heads_here, bool(packed), steps, context),
        out_shape=[jax.ShapeDtypeStruct((rows, wide), F32)] * count
        + [jax.ShapeDtypeStruct((rows, head_dim), F32)] * 2,
        in_specs=[VMEM] * 3 + [SMEM] + [VMEM] * len(packed),
        out_specs=[VMEM] * (count + 2),
        scratch_shapes=[pltpu.VMEM((rows, width), BF16)],
        compiler_params=params(8 * MIB),
        cost_estimate=cost(2 * rows * weight.size, size),
        name="project",
    )(x, attn_gain.reshape(1, width), weight, lengths, *packed)


def folded(used):
    return used % LANES == LANES // 2


def fold(columns, used):
    rows = columns.shape[0]
    if not folded(used):
        return columns
    parts = [columns[:, i : i + LANES] for i in range(0, used - LANES // 2, LANES)]
    rest = columns[:, used - LANES // 2 : used]
    return jnp.concatenate(
        parts + [jnp.concatenate([rest[: rows // 2], rest[rows // 2 :]], axis=1)], axis=0
    )


def unfold(block, rows, used):
    if not folded(used):
        return block
    full = used // LANES
    parts = [block[i * rows : (i + 1) * rows] for i in range(full)]
    rest = block[full * rows :]
    half = LANES // 2
    return jnp.concatenate(
        parts + [jnp.concatenate([rest[:, :half], rest[:, half:]], axis=0)], axis=1
    )


def norm_kernel(used, model_width, *refs):
    pieces, out = refs[:-1], refs[-1]
    total = pieces[0][...]
    for piece in pieces[1:]:
        total = total + piece[...]
    factor = lax.rsqrt(total[:, used : used + 1] * (1.0 / model_width) + EPSILON)
    united = fold(total * factor, used).astype(BF16)
    for target in range(out.shape[0]):
        out[target] = united


def norm_copies(pieces, used, model_width):
    rows, wide = pieces[0].shape
    if folded(used):
        rows, wide = rows * used // LANES, LANES
    return pl.pallas_call(
        functools.partial(norm_kernel, used, model_width),
        out_shape=jax.ShapeDtypeStruct((lax.axis_size("ctx"), rows, wide), BF16),
        in_specs=[VMEM] * len(pieces),
        out_specs=VMEM,
        compiler_params=params(8 * MIB),
        name="norm",
    )(*pieces)


def split3(value):
    first = value.astype(BF16).astype(F32)
    second = (value - first).astype(BF16).astype(F32)
    return first, second, value - first - second


def near_block(query, fresh_key, fresh_value, keys, values, head, heads, steps, lengths):
    owned, slots_all, _ = keys.shape
    block = query.shape[0]
    rows = fresh_key.shape[0]
    mine = lax.axis_index("ctx")

    def iota(shape, axis):
        return lax.broadcasted_iota(jnp.int32, shape, axis)

    query_place = iota((block, 1), 0) % (owned * steps)
    sequence = query_place // steps
    step = query_place % steps
    slot = iota((1, slots_all), 1)
    fresh_row = iota((1, rows), 1)
    fresh_here = (fresh_row // steps == mine * owned + sequence) & (fresh_row % steps <= step)
    fresh_scores = lax.dot_general(query, fresh_key, NT, preferred_element_type=F32)
    scores = [jnp.where(fresh_here, fresh_scores, MASKED)]
    highest = jnp.max(scores[0], axis=-1, keepdims=True)
    for s in range(owned):
        found = lax.dot_general(query, keys[s], NT, preferred_element_type=F32)
        live = (sequence == s) & (slot % heads == head)
        live = live & (slot // heads < lengths[mine * owned + s])
        found = jnp.where(live, found, MASKED)
        scores.append(found)
        highest = jnp.maximum(highest, jnp.max(found, axis=-1, keepdims=True))
    total = jnp.zeros((block, 1), F32)
    result = jnp.zeros((block, fresh_value.shape[1]), F32)
    for found, value in zip(scores, [fresh_value] + [values[s] for s in range(owned)]):
        weights = jnp.exp(found - highest).astype(BF16)
        total = total + jnp.sum(weights.astype(F32), axis=-1, keepdims=True)
        result = result + jnp.dot(weights, value, preferred_element_type=F32)
    return highest, total, result


def attend_kernel(
    columns,
    group,
    owned,
    lengths,
    united,
    cosine,
    sine,
    keys,
    values,
    slot_keys,
    slot_values,
    packet,
    near_sums,
    near_maxima,
    near_totals,
    query_buf,
    score_buf,
):
    chunks = united.shape[0]
    rows = cosine.shape[0]
    heads, context, head_dim = keys.shape
    per_dest = rows // chunks
    block = per_dest * group
    tile = min(512, context)
    tiles = context // tile
    cos = cosine[...]
    sin = sine[...]
    mine = lax.axis_index("ctx")

    def rotated(vectors):
        return vectors * cos + pltpu.roll(vectors, head_dim // 2, 1) * sin

    fresh = []
    sources = [
        unfold(united[chunk].astype(F32), rows, heads * columns) for chunk in range(chunks)
    ]
    for head in range(heads):
        first = head * columns
        whole = jnp.concatenate([x[:, first : first + columns] for x in sources], axis=1)
        for j in range(group):
            query = rotated(whole[:, j * head_dim : (j + 1) * head_dim]) * head_dim ** (-0.5)
            for dest in range(chunks):
                start = dest * block + j * per_dest
                query_buf[head, start : start + per_dest, :] = query[
                    dest * per_dest : (dest + 1) * per_dest
                ]
        new_key = rotated(whole[:, group * head_dim : (group + 1) * head_dim])
        new_value = whole[:, (group + 1) * head_dim :]
        fresh.append((new_key.astype(BF16), new_value.astype(BF16)))

    lane = lax.broadcasted_iota(jnp.int32, (chunks * block, LANES), 1)
    table = jnp.zeros((chunks * block, LANES), F32)
    for head in range(heads):
        query = query_buf[head].astype(BF16)
        highest = None
        for step in range(tiles):
            span = slice(step * tile, (step + 1) * tile)
            scores = lax.dot_general(
                query, keys[head, span, :], NT, preferred_element_type=F32
            )
            score_buf[:, span] = scores
            for part in range(tile // LANES):
                piece = scores[:, part * LANES : (part + 1) * LANES]
                highest = piece if highest is None else jnp.maximum(highest, piece)
        maxima = jnp.max(highest, axis=-1, keepdims=True)
        sums = jnp.zeros((chunks * block, head_dim), F32)
        totals = jnp.zeros((chunks * block, LANES), F32)
        for step in range(tiles):
            span = slice(step * tile, (step + 1) * tile)
            weights = jnp.exp(score_buf[:, span] - maxima).astype(BF16)
            sums = sums + jnp.dot(weights, values[head, span, :], preferred_element_type=F32)
            wide = weights.astype(F32)
            for part in range(tile // LANES):
                totals = totals + wide[:, part * LANES : (part + 1) * LANES]
        total = jnp.sum(totals, axis=-1, keepdims=True)
        for index, piece in enumerate(split3(maxima) + split3(total)):
            table = jnp.where(lane == head * 8 + index, piece, table)
        rounded = sums.astype(BF16)
        for dest in range(chunks):
            packet[dest, head * block : (head + 1) * block] = rounded[
                dest * block : (dest + 1) * block
            ]
        own_query = query_buf[head, pl.ds(pl.multiple_of(mine * block, block), block), :]
        near_max, near_total, near_sum = near_block(
            own_query.astype(BF16),
            *fresh[head],
            slot_keys,
            slot_values,
            head,
            heads,
            per_dest // owned,
            lengths,
        )
        span = slice(head * block, (head + 1) * block)
        near_sums[span, :] = near_sum
        near_maxima[span, :] = jnp.broadcast_to(near_max, (block, head_dim))
        near_totals[span, :] = jnp.broadcast_to(near_total, (block, head_dim))
    low = heads * block
    pieces = packet.shape[1] - low
    turned = jnp.transpose(table)[:pieces]
    for dest in range(chunks):
        packet[dest, low:, :block] = turned[:, dest * block : (dest + 1) * block].astype(BF16)


def attend(united, columns, cosine, sine, keys, values, lengths, slot_keys, slot_values):
    chunks = united.shape[0]
    rows = cosine.shape[0]
    heads, context, head_dim = keys.shape
    owned, slots, _, _ = slot_keys.shape
    group = columns * chunks // head_dim - 2
    block = rows // chunks * group
    size = keys.size * 2
    flat = chunks * block
    near = jax.ShapeDtypeStruct((heads * block, head_dim), F32)
    return pl.pallas_call(
        functools.partial(attend_kernel, columns, group, owned),
        out_shape=[
            jax.ShapeDtypeStruct((chunks, heads * block + round_up(heads * 8, 16), head_dim), BF16),
            near,
            near,
            near,
        ],
        in_specs=[SMEM] + [VMEM] * 7,
        out_specs=[VMEM] * 4,
        scratch_shapes=[
            pltpu.VMEM((heads, flat, head_dim), F32),
            pltpu.VMEM((flat, context), F32),
        ],
        compiler_params=params(flat * context * 4 + 12 * MIB),
        cost_estimate=cost(4 * heads * flat * context * head_dim, 2 * size, heads * flat * context),
        name="attend",
    )(
        lengths,
        united,
        cosine,
        sine,
        keys,
        values,
        slot_keys.reshape(owned, slots * heads, head_dim),
        slot_values.reshape(owned, slots * heads, head_dim),
    )


def merge_kernel(group, parts, near_sums, near_maxima, near_totals, out, places, stats):
    chunks = parts.shape[0]
    per_dest = out.shape[1]
    block = per_dest * group
    queries, head_dim = near_sums.shape
    heads = queries // block
    highest = near_maxima[...][:, :1]
    maxima, totals = [], []
    pieces = parts.shape[1] - queries
    for source in range(chunks):
        stats[source * pieces : (source + 1) * pieces, :] = parts[source, queries:, :].astype(F32)
    turned = jnp.transpose(stats[...])[:block]
    for source in range(chunks):
        m, t = [], []
        for head in range(heads):
            column = source * pieces + head * 8
            get = lambda k: turned[:, column + k : column + k + 1]
            m.append(get(0) + get(1) + get(2))
            t.append(get(3) + get(4) + get(5))
        maxima.append(jnp.concatenate(m, axis=0))
        totals.append(jnp.concatenate(t, axis=0))
        highest = jnp.maximum(highest, maxima[-1])
    scale = jnp.exp(near_maxima[...][:, :1] - highest)
    numerator = near_sums[...] * scale
    denominator = near_totals[...][:, :1] * scale
    for source in range(chunks):
        scale = jnp.exp(maxima[source] - highest)
        numerator = numerator + parts[source, :queries, :].astype(F32) * scale
        denominator = denominator + totals[source] * scale
    attention = numerator / denominator
    for index in range(heads * group):
        places[:, index * head_dim : (index + 1) * head_dim] = attention[
            index * per_dest : (index + 1) * per_dest
        ]
    rounded = places[...].astype(BF16)
    for target in range(chunks):
        out[target] = rounded


def merge_copies(parts, sums, maxima, totals, group, per_dest):
    chunks = parts.shape[0]
    queries, head_dim = sums.shape
    heads = queries // (per_dest * group)
    width = heads * group * head_dim
    return pl.pallas_call(
        functools.partial(merge_kernel, group),
        out_shape=jax.ShapeDtypeStruct((chunks, per_dest, width), BF16),
        in_specs=[VMEM] * 4,
        out_specs=VMEM,
        scratch_shapes=[
            pltpu.VMEM((per_dest, width), F32),
            pltpu.VMEM((chunks * (parts.shape[1] - queries), head_dim), F32),
        ],
        compiler_params=params(12 * MIB),
        name="merge",
    )(parts, sums, maxima, totals)


def output_kernel(x, weight, *refs):
    chunks, per_dest, depth = x.shape
    rows_f32, total = refs[-2:]
    outs = refs[:-2]
    count = len(outs)
    for chunk in range(chunks):
        rows_f32[chunk * per_dest : (chunk + 1) * per_dest, :] = x[chunk].astype(F32)
    total[...] = jnp.dot(
        rows_f32[...].astype(BF16), weight[...], preferred_element_type=F32
    )
    here = lax.axis_index("head")
    height = total.shape[0] // count
    for shift in range(count):
        first = pl.multiple_of(partner(here, shift, count) * height, height)
        outs[shift][...] = total[pl.ds(first, height), :].astype(BF16)


def project_out(x, weight):
    count = lax.axis_size("head")
    chunks, per_dest, depth = x.shape
    rows = chunks * per_dest
    width = weight.shape[1]
    return pl.pallas_call(
        output_kernel,
        out_shape=[jax.ShapeDtypeStruct((rows // count, width), BF16)] * count,
        in_specs=[VMEM, VMEM],
        out_specs=[VMEM] * count,
        scratch_shapes=[pltpu.VMEM((rows, depth), F32), pltpu.VMEM((rows, width), F32)],
        compiler_params=params(8 * MIB),
        cost_estimate=cost(2 * rows * weight.size, weight.size * 2),
        name="output",
    )(x, weight)


def body(
    token_ids,
    suffix_lengths,
    embedding,
    attn_gain,
    qkv_weight,
    out_weight,
    prefix_keys,
    prefix_values,
    suffix_keys,
    suffix_values,
):
    steps, batch = token_ids.shape
    rows = steps * batch
    n_ctx = lax.axis_size("ctx")
    n_head = lax.axis_size("head")
    heads, block_context, head_dim = prefix_keys.shape
    width = embedding.shape[1]
    columns = qkv_weight.shape[2]
    group = columns * n_ctx // head_dim - 2
    context = block_context * n_ctx
    capacity = 2 * rows // n_ctx
    qkv_weight = jnp.transpose(qkv_weight, (1, 2, 0))
    if embedding.shape[0] % 8 == 0 and capacity % 8 == 0:
        packed, places, crowded = lookup_packed(token_ids, embedding, capacity)

        def rest():
            found = lookup_rest(token_ids, places, embedding)
            return exchange(join_copies(exchange(found, "ctx")), "ctx")

        def nothing():
            return jnp.zeros((n_ctx, rows, width // n_ctx), BF16)

        features = lax.cond(crowded[0] > 0, rest, nothing)
        packed = exchange(spread(packed, features, 4 * qkv_weight.size), "ctx")
        packed = (packed, places)
    else:
        joined = join_copies(exchange(lookup_all(token_ids, embedding), "ctx"))
        features, packed = exchange(joined, "ctx"), ()
    *pieces, cosine, sine = project(
        features, attn_gain, qkv_weight, suffix_lengths, steps, context, head_dim, packed
    )
    pieces = send_pieces(pieces, "head")
    united = norm_copies(pieces, heads * columns, width * n_head)
    united = exchange(united, "ctx")
    packet, sums, maxima, totals = attend(
        united,
        columns,
        cosine,
        sine,
        prefix_keys,
        prefix_values,
        suffix_lengths,
        suffix_keys,
        suffix_values,
    )
    parts = exchange(packet, "ctx")
    attention = merge_copies(parts, sums, maxima, totals, group, rows // n_ctx)
    attention = exchange(attention, "ctx")
    pieces = send_pieces(project_out(attention, out_weight), "head")
    result = pieces[0].astype(F32)
    for piece in pieces[1:]:
        result = result + piece.astype(F32)
    return result.astype(BF16).reshape(batch // n_head, steps, -1)


def solution(mesh):
    placed = (
        P(),
        P(),
        P("ctx", "head"),
        P("head"),
        P("head", None, "ctx"),
        P("head", "ctx"),
        P("head", "ctx", None),
        P("head", "ctx", None),
        P("ctx", None, "head", None),
        P("ctx", None, "head", None),
    )
    return jax.shard_map(
        body, mesh=mesh, in_specs=placed, out_specs=P("head", None, "ctx"), check_vma=False
    )
```

```python
import functools

import jax
import jax.numpy as jnp
import numpy as np
from jax import lax
from jax.experimental import pallas as pl
from jax.experimental.pallas import tpu as pltpu
from jax.sharding import PartitionSpec as P

EPSILON = 1e-05
ROTARY_THETA = 500000.0
MASKED = -1e30
BF16 = jnp.bfloat16
F32 = jnp.float32
LANES = 128
MIB = 1 << 20
VMEM = pl.BlockSpec(memory_space=pltpu.VMEM)
SMEM = pl.BlockSpec(memory_space=pltpu.SMEM)
HBM = pl.BlockSpec(memory_space=pl.ANY)
NT = (((1,), (1,)), ((), ()))


def round_up(value, unit):
    return -(-value // unit) * unit


def params(limit):
    return pltpu.CompilerParams(vmem_limit_bytes=min(limit, 60 * MIB))


def cost(flops, moved, transcendentals=0):
    return pl.CostEstimate(flops=flops, bytes_accessed=moved, transcendentals=transcendentals)


def exchange(blocks, axis):
    return lax.all_to_all(blocks, axis, 0, 0)


def partner(here, shift, count):
    if count & (count - 1) == 0:
        return here ^ shift
    return (here + shift) % count


def send_pieces(pieces, axis):
    count = lax.axis_size(axis)
    received = [pieces[0]]
    for shift in range(1, count):
        pairs = [(i, partner(i, shift, count)) for i in range(count)]
        received.append(lax.ppermute(pieces[shift], axis, pairs))
    return received


def token_at(tokens, row):
    steps = tokens.shape[0]
    return tokens[row % steps, row // steps]


def assign_slots(tokens, rows, owners, local_rows, capacity):
    lanes = round_up(rows, LANES)
    down = lax.broadcasted_iota(jnp.int32, (rows, lanes), 0)
    across = lax.broadcasted_iota(jnp.int32, (rows, lanes), 1)
    column = jnp.zeros((rows, lanes), jnp.int32)
    line = jnp.full((rows, lanes), -1, jnp.int32)
    for row in range(rows):
        token = token_at(tokens, row)
        column = jnp.where(down == row, token, column)
        line = jnp.where(across == row, token, line)
    owner_column = jnp.zeros((rows, lanes), F32)
    owner_line = jnp.zeros((rows, lanes), F32)
    for owner in range(1, owners):
        owner_column += jnp.where(column >= owner * local_rows, 1.0, 0.0)
        owner_line += jnp.where(line >= owner * local_rows, 1.0, 0.0)
    same = jnp.where(column == line, 1.0, 0.0)
    index = across.astype(F32)
    earliest = jnp.min(jnp.where(same > 0, index, float(lanes)), axis=1, keepdims=True)
    repeated = jnp.max(jnp.where(down < across, same, 0.0), axis=0, keepdims=True)
    counted = jnp.where((repeated == 0) & (across < rows) & (index < earliest), 1.0, 0.0)
    slot = jnp.sum(jnp.where(owner_column == owner_line, counted, 0.0), axis=1, keepdims=True)
    place = jnp.where(slot < capacity, owner_column[:, :1] * capacity + slot, -1.0)
    first = earliest == down[:, :1].astype(F32)
    return place, first


def rotary_tables(lengths, steps, rows, context, head_dim):
    half = head_dim // 2
    down = lax.broadcasted_iota(jnp.int32, (rows, head_dim), 0)
    across = lax.broadcasted_iota(jnp.int32, (1, head_dim), 1)
    frequency = jnp.zeros((1, head_dim), F32)
    for i in range(half):
        value = float(np.float32(ROTARY_THETA ** (-2.0 * i / head_dim)))
        frequency = jnp.where(across % half == i, value, frequency)
    length = jnp.zeros((rows, head_dim), jnp.int32)
    for sequence in range(rows // steps):
        length = jnp.where(down // steps == sequence, lengths[sequence], length)
    positions = (context + length + down % steps).astype(F32)
    angles = positions * frequency
    sine = jnp.sin(angles)
    return jnp.cos(angles), jnp.where(across < half, -sine, sine)


def fetch_rows(tokens, table, blocks, rows_f32, sem, between=None):
    rows = rows_f32.shape[0]
    local_rows = table.shape[0]
    base = lax.axis_index("ctx") * local_rows

    def find(row):
        offset = token_at(tokens, row) - base
        return offset, (offset >= 0) & (offset < local_rows)

    def copy(row, offset):
        start = pl.multiple_of((offset // 8) * 8, 8)
        return pltpu.make_async_copy(
            table.at[pl.ds(start, 8), :], blocks.at[row], sem.at[row]
        )

    for row in range(rows):
        offset, inside = find(row)

        @pl.when(inside)
        def _():
            copy(row, offset).start()

    rows_f32[...] = jnp.zeros_like(rows_f32)
    result = None if between is None else between()
    sublane = lax.broadcasted_iota(jnp.int32, (8, 1), 0)
    for row in range(rows):
        offset, inside = find(row)

        @pl.when(inside)
        def _():
            copy(row, offset).wait()
            picked = jnp.where(sublane == offset % 8, blocks[row].astype(F32), 0.0)
            rows_f32[row : row + 1, :] = jnp.sum(picked, axis=0, keepdims=True)

    return result


def lookup_kernel(
    owners, tokens, table, packed, places, crowded, blocks, rows_f32, sem
):
    capacity, _ = packed.shape
    rows = rows_f32.shape[0]

    def between():
        return assign_slots(tokens, rows, owners, table.shape[0], capacity)

    place, first = fetch_rows(tokens, table, blocks, rows_f32, sem, between)
    places[...] = jnp.broadcast_to(place, places.shape)
    crowded[0] = jnp.max(jnp.where(place < 0, 1, 0))
    slot = lax.broadcasted_iota(jnp.int32, (rows, capacity), 1) + lax.axis_index("ctx") * capacity
    chosen = jnp.where((place == slot.astype(F32)) & first, 1.0, 0.0).astype(BF16)
    packed[...] = lax.dot_general(
        chosen, rows_f32[...].astype(BF16), (((0,), (0,)), ((), ())), preferred_element_type=F32
    ).astype(BF16)


def rest_kernel(tokens, places, table, out, blocks, rows_f32, sem):
    chunks, rows, width = out.shape
    fetch_rows(tokens, table, blocks, rows_f32, sem)
    left = places[...][:, :1] < 0
    for chunk in range(chunks):
        found = rows_f32[:, chunk * width : (chunk + 1) * width]
        out[chunk] = jnp.where(left, found, 0.0).astype(BF16)


def fetch_scratch(rows, width):
    return [
        pltpu.VMEM((rows, 8, width), BF16),
        pltpu.VMEM((rows, width), F32),
        pltpu.SemaphoreType.DMA((rows,)),
    ]


def spread_kernel(block, first, out):
    for target in range(out.shape[0]):
        out[target] = block[...]


def spread(block, first, hint):
    count = lax.axis_size("ctx")
    return pl.pallas_call(
        spread_kernel,
        out_shape=jax.ShapeDtypeStruct((count,) + block.shape, block.dtype),
        in_specs=[VMEM, HBM],
        out_specs=VMEM,
        compiler_params=params(8 * MIB),
        cost_estimate=cost(400 * hint, hint),
        name="spread",
    )(block, first)


def lookup_packed(token_ids, embedding, capacity):
    steps, batch = token_ids.shape
    rows = steps * batch
    owners = lax.axis_size("ctx")
    _, width = embedding.shape
    return pl.pallas_call(
        functools.partial(lookup_kernel, owners),
        out_shape=[
            jax.ShapeDtypeStruct((capacity, width), BF16),
            jax.ShapeDtypeStruct((rows, LANES), F32),
            jax.ShapeDtypeStruct((1,), jnp.int32),
        ],
        in_specs=[SMEM, HBM],
        out_specs=[VMEM, VMEM, SMEM],
        scratch_shapes=fetch_scratch(rows, width),
        compiler_params=params(6 * rows * width * 8),
        cost_estimate=cost(rows * width, rows * width * 16),
        name="lookup",
    )(token_ids, embedding)


def lookup_rest(token_ids, places, embedding):
    rows = places.shape[0]
    chunks = lax.axis_size("ctx")
    _, width = embedding.shape
    return pl.pallas_call(
        rest_kernel,
        out_shape=jax.ShapeDtypeStruct((chunks, rows, width // chunks), BF16),
        in_specs=[SMEM, VMEM, HBM],
        out_specs=VMEM,
        scratch_shapes=fetch_scratch(rows, width),
        compiler_params=params(6 * rows * width * 8),
        name="rest",
    )(token_ids, places, embedding)


def lookup_all(token_ids, embedding):
    steps, batch = token_ids.shape
    rows = steps * batch
    chunks = lax.axis_size("ctx")
    local_rows, width = embedding.shape
    offsets = token_ids.T.reshape(rows) - lax.axis_index("ctx") * local_rows
    inside = (offsets >= 0) & (offsets < local_rows)
    picked = jnp.take(embedding, jnp.clip(offsets, 0, local_rows - 1), axis=0)
    picked = jnp.where(inside[:, None], picked, jnp.zeros((), BF16))
    return jnp.swapaxes(picked.reshape(rows, chunks, width // chunks), 0, 1)


def join_kernel(parts, out):
    total = parts[0].astype(F32)
    for source in range(1, parts.shape[0]):
        total = total + parts[source].astype(F32)
    joined = total.astype(BF16)
    for target in range(out.shape[0]):
        out[target] = joined


def join_copies(parts):
    return pl.pallas_call(
        join_kernel,
        out_shape=jax.ShapeDtypeStruct(parts.shape, BF16),
        in_specs=[VMEM],
        out_specs=VMEM,
        compiler_params=params(8 * MIB),
        name="join",
    )(parts)


def project_kernel(heads_here, packed, steps, context, x, gain, weight, lengths, *refs):
    if packed:
        slots, places, *refs = refs
    count = weight.shape[0] // heads_here
    outs, (cosine, sine, scaled) = refs[:count], refs[count:]
    chunks, rows, chunk_width = x.shape
    if packed:
        owners, capacity, width = slots.shape
        held = slots[...].astype(F32).reshape(owners * capacity, width).astype(BF16)
        slot = lax.broadcasted_iota(jnp.int32, (rows, owners * capacity), 1).astype(F32)
        chosen = jnp.where(places[...][:, :1] == slot, 1.0, 0.0).astype(BF16)
    columns = weight.shape[1]
    here = lax.axis_index("head")
    squares = jnp.zeros((rows, 1), F32)
    for chunk in range(chunks):
        span = slice(chunk * chunk_width, (chunk + 1) * chunk_width)
        features = x[chunk].astype(F32)
        if packed:
            features += jnp.dot(chosen, held[:, span], preferred_element_type=F32)
        squares = squares + jnp.sum(features * features, axis=-1, keepdims=True)
        scaled[:, span] = (features * gain[:, span]).astype(BF16)
    used = heads_here * columns
    rest = outs[0].shape[1] - used
    for shift in range(count):
        first = partner(here, shift, count) * heads_here
        products = [
            lax.dot_general(scaled[...], weight[first + head], NT, preferred_element_type=F32)
            for head in range(heads_here)
        ]
        outs[shift][...] = jnp.concatenate(
            products + [jnp.broadcast_to(squares, (rows, rest))], axis=1
        )
    cosine[...], sine[...] = rotary_tables(lengths, steps, rows, context, cosine.shape[1])


def project(x, attn_gain, weight, lengths, steps, context, head_dim, packed):
    count = lax.axis_size("head")
    chunks, rows, chunk_width = x.shape
    heads, columns, width = weight.shape
    heads_here = heads // count
    wide = round_up(heads_here * columns + 1, LANES)
    size = weight.size * 2
    return pl.pallas_call(
        functools.partial(project_kernel, heads_here, bool(packed), steps, context),
        out_shape=[jax.ShapeDtypeStruct((rows, wide), F32)] * count
        + [jax.ShapeDtypeStruct((rows, head_dim), F32)] * 2,
        in_specs=[VMEM] * 3 + [SMEM] + [VMEM] * len(packed),
        out_specs=[VMEM] * (count + 2),
        scratch_shapes=[pltpu.VMEM((rows, width), BF16)],
        compiler_params=params(8 * MIB),
        cost_estimate=cost(2 * rows * weight.size, size),
        name="project",
    )(x, attn_gain.reshape(1, width), weight, lengths, *packed)


def folded(used):
    return used % LANES == LANES // 2


def fold(columns, used):
    rows = columns.shape[0]
    if not folded(used):
        return columns
    parts = [columns[:, i : i + LANES] for i in range(0, used - LANES // 2, LANES)]
    rest = columns[:, used - LANES // 2 : used]
    return jnp.concatenate(
        parts + [jnp.concatenate([rest[: rows // 2], rest[rows // 2 :]], axis=1)], axis=0
    )


def unfold(block, rows, used):
    if not folded(used):
        return block
    full = used // LANES
    parts = [block[i * rows : (i + 1) * rows] for i in range(full)]
    rest = block[full * rows :]
    half = LANES // 2
    return jnp.concatenate(
        parts + [jnp.concatenate([rest[:, :half], rest[:, half:]], axis=0)], axis=1
    )


def norm_kernel(used, model_width, *refs):
    pieces, out = refs[:-1], refs[-1]
    total = pieces[0][...]
    for piece in pieces[1:]:
        total = total + piece[...]
    factor = lax.rsqrt(total[:, used : used + 1] * (1.0 / model_width) + EPSILON)
    united = fold(total * factor, used).astype(BF16)
    for target in range(out.shape[0]):
        out[target] = united


def norm_copies(pieces, used, model_width):
    rows, wide = pieces[0].shape
    if folded(used):
        rows, wide = rows * used // LANES, LANES
    return pl.pallas_call(
        functools.partial(norm_kernel, used, model_width),
        out_shape=jax.ShapeDtypeStruct((lax.axis_size("ctx"), rows, wide), BF16),
        in_specs=[VMEM] * len(pieces),
        out_specs=VMEM,
        compiler_params=params(8 * MIB),
        name="norm",
    )(*pieces)


def split3(value):
    first = value.astype(BF16).astype(F32)
    second = (value - first).astype(BF16).astype(F32)
    return first, second, value - first - second


def near_block(query, fresh_key, fresh_value, keys, values, heads, steps, lengths):
    owned, slots_all, _ = keys.shape
    block = query.shape[0] // heads
    rows = fresh_key.shape[0] // heads
    mine = lax.axis_index("ctx")

    def iota(shape, axis):
        return lax.broadcasted_iota(jnp.int32, shape, axis)

    place = iota((heads * block, 1), 0)
    head = place // block
    sequence = place % (owned * steps) // steps
    step = place % steps
    slot = iota((1, slots_all), 1)
    fresh_row = iota((1, heads * rows), 1)
    fresh_here = (fresh_row // steps == head * (rows // steps) + mine * owned + sequence) & (
        fresh_row % steps <= step
    )
    fresh_scores = lax.dot_general(query, fresh_key, NT, preferred_element_type=F32)
    scores = [jnp.where(fresh_here, fresh_scores, MASKED)]
    highest = jnp.max(scores[0], axis=-1, keepdims=True)
    for s in range(owned):
        found = lax.dot_general(query, keys[s], NT, preferred_element_type=F32)
        live = (sequence == s) & (slot % heads == head)
        live = live & (slot // heads < lengths[mine * owned + s])
        found = jnp.where(live, found, MASKED)
        scores.append(found)
        highest = jnp.maximum(highest, jnp.max(found, axis=-1, keepdims=True))
    total = jnp.zeros((heads * block, 1), F32)
    result = jnp.zeros((heads * block, fresh_value.shape[1]), F32)
    for found, value in zip(scores, [fresh_value] + [values[s] for s in range(owned)]):
        weights = jnp.exp(found - highest).astype(BF16)
        total = total + jnp.sum(weights.astype(F32), axis=-1, keepdims=True)
        result = result + jnp.dot(weights, value, preferred_element_type=F32)
    return highest, total, result


def attend_kernel(
    columns,
    group,
    owned,
    lengths,
    united,
    cosine,
    sine,
    keys,
    values,
    slot_keys,
    slot_values,
    packet,
    near_sums,
    near_maxima,
    near_totals,
    query_buf,
    score_buf,
):
    chunks = united.shape[0]
    rows = cosine.shape[0]
    heads, context, head_dim = keys.shape
    per_dest = rows // chunks
    block = per_dest * group
    tile = min(512, context)
    tiles = context // tile
    cos = cosine[...]
    sin = sine[...]
    mine = lax.axis_index("ctx")

    def rotated(vectors):
        return vectors * cos + pltpu.roll(vectors, head_dim // 2, 1) * sin

    fresh = []
    sources = [
        unfold(united[chunk].astype(F32), rows, heads * columns) for chunk in range(chunks)
    ]
    for head in range(heads):
        first = head * columns
        whole = jnp.concatenate([x[:, first : first + columns] for x in sources], axis=1)
        for j in range(group):
            query = rotated(whole[:, j * head_dim : (j + 1) * head_dim]) * head_dim ** (-0.5)
            for dest in range(chunks):
                start = dest * block + j * per_dest
                query_buf[head, start : start + per_dest, :] = query[
                    dest * per_dest : (dest + 1) * per_dest
                ]
        new_key = rotated(whole[:, group * head_dim : (group + 1) * head_dim])
        new_value = whole[:, (group + 1) * head_dim :]
        fresh.append((new_key.astype(BF16), new_value.astype(BF16)))

    lane = lax.broadcasted_iota(jnp.int32, (chunks * block, LANES), 1)
    table = jnp.zeros((chunks * block, LANES), F32)
    for head in range(heads):
        query = query_buf[head].astype(BF16)
        highest = None
        for step in range(tiles):
            span = slice(step * tile, (step + 1) * tile)
            scores = lax.dot_general(
                query, keys[head, span, :], NT, preferred_element_type=F32
            )
            score_buf[:, span] = scores
            for part in range(tile // LANES):
                piece = scores[:, part * LANES : (part + 1) * LANES]
                highest = piece if highest is None else jnp.maximum(highest, piece)
        maxima = jnp.max(highest, axis=-1, keepdims=True)
        both = jnp.zeros((chunks * block, head_dim + LANES), F32)
        ones = jnp.ones((tile, LANES), BF16)
        for step in range(tiles):
            span = slice(step * tile, (step + 1) * tile)
            weights = jnp.exp(score_buf[:, span] - maxima).astype(BF16)
            extended = jnp.concatenate([values[head, span, :], ones], axis=1)
            both = both + jnp.dot(weights, extended, preferred_element_type=F32)
        sums, total = both[:, :head_dim], both[:, head_dim:]
        for index, piece in enumerate(split3(maxima) + split3(total)):
            table = jnp.where(lane == head * 8 + index, piece, table)
        rounded = sums.astype(BF16)
        for dest in range(chunks):
            packet[dest, head * block : (head + 1) * block] = rounded[
                dest * block : (dest + 1) * block
            ]
    own = pl.ds(pl.multiple_of(mine * block, block), block)
    near_max, near_total, near_sum = near_block(
        jnp.concatenate([query_buf[head, own, :] for head in range(heads)], axis=0).astype(BF16),
        jnp.concatenate([key for key, value in fresh], axis=0),
        jnp.concatenate([value for key, value in fresh], axis=0),
        slot_keys,
        slot_values,
        heads,
        per_dest // owned,
        lengths,
    )
    near_sums[...] = near_sum
    near_maxima[...] = jnp.broadcast_to(near_max, near_maxima.shape)
    near_totals[...] = jnp.broadcast_to(near_total, near_totals.shape)
    low = heads * block
    pieces = packet.shape[1] - low
    turned = jnp.transpose(table)[:pieces]
    for dest in range(chunks):
        packet[dest, low:, :block] = turned[:, dest * block : (dest + 1) * block].astype(BF16)


def attend(united, columns, cosine, sine, keys, values, lengths, slot_keys, slot_values):
    chunks = united.shape[0]
    rows = cosine.shape[0]
    heads, context, head_dim = keys.shape
    owned, slots, _, _ = slot_keys.shape
    group = columns * chunks // head_dim - 2
    block = rows // chunks * group
    size = keys.size * 2
    flat = chunks * block
    near = jax.ShapeDtypeStruct((heads * block, head_dim), F32)
    return pl.pallas_call(
        functools.partial(attend_kernel, columns, group, owned),
        out_shape=[
            jax.ShapeDtypeStruct((chunks, heads * block + round_up(heads * 8, 16), head_dim), BF16),
            near,
            near,
            near,
        ],
        in_specs=[SMEM] + [VMEM] * 7,
        out_specs=[VMEM] * 4,
        scratch_shapes=[
            pltpu.VMEM((heads, flat, head_dim), F32),
            pltpu.VMEM((flat, context), F32),
        ],
        compiler_params=params(flat * context * 4 + 12 * MIB),
        cost_estimate=cost(4 * heads * flat * context * head_dim, 2 * size, heads * flat * context),
        name="attend",
    )(
        lengths,
        united,
        cosine,
        sine,
        keys,
        values,
        slot_keys.reshape(owned, slots * heads, head_dim),
        slot_values.reshape(owned, slots * heads, head_dim),
    )


def merge_kernel(group, parts, near_sums, near_maxima, near_totals, out, places, stats):
    chunks = parts.shape[0]
    per_dest = out.shape[1]
    block = per_dest * group
    queries, head_dim = near_sums.shape
    heads = queries // block
    highest = near_maxima[...][:, :1]
    maxima, totals = [], []
    pieces = parts.shape[1] - queries
    for source in range(chunks):
        stats[source * pieces : (source + 1) * pieces, :] = parts[source, queries:, :].astype(F32)
    turned = jnp.transpose(stats[...])[:block]
    for source in range(chunks):
        m, t = [], []
        for head in range(heads):
            column = source * pieces + head * 8
            get = lambda k: turned[:, column + k : column + k + 1]
            m.append(get(0) + get(1) + get(2))
            t.append(get(3) + get(4) + get(5))
        maxima.append(jnp.concatenate(m, axis=0))
        totals.append(jnp.concatenate(t, axis=0))
        highest = jnp.maximum(highest, maxima[-1])
    scale = jnp.exp(near_maxima[...][:, :1] - highest)
    numerator = near_sums[...] * scale
    denominator = near_totals[...][:, :1] * scale
    for source in range(chunks):
        scale = jnp.exp(maxima[source] - highest)
        numerator = numerator + parts[source, :queries, :].astype(F32) * scale
        denominator = denominator + totals[source] * scale
    attention = numerator / denominator
    for index in range(heads * group):
        places[:, index * head_dim : (index + 1) * head_dim] = attention[
            index * per_dest : (index + 1) * per_dest
        ]
    rounded = places[...].astype(BF16)
    for target in range(chunks):
        out[target] = rounded


def merge_copies(parts, sums, maxima, totals, group, per_dest):
    chunks = parts.shape[0]
    queries, head_dim = sums.shape
    heads = queries // (per_dest * group)
    width = heads * group * head_dim
    return pl.pallas_call(
        functools.partial(merge_kernel, group),
        out_shape=jax.ShapeDtypeStruct((chunks, per_dest, width), BF16),
        in_specs=[VMEM] * 4,
        out_specs=VMEM,
        scratch_shapes=[
            pltpu.VMEM((per_dest, width), F32),
            pltpu.VMEM((chunks * (parts.shape[1] - queries), head_dim), F32),
        ],
        compiler_params=params(12 * MIB),
        name="merge",
    )(parts, sums, maxima, totals)


def output_kernel(x, weight, *refs):
    chunks, per_dest, depth = x.shape
    rows_f32, total = refs[-2:]
    outs = refs[:-2]
    count = len(outs)
    for chunk in range(chunks):
        rows_f32[chunk * per_dest : (chunk + 1) * per_dest, :] = x[chunk].astype(F32)
    total[...] = jnp.dot(
        rows_f32[...].astype(BF16), weight[...], preferred_element_type=F32
    )
    here = lax.axis_index("head")
    height = total.shape[0] // count
    for shift in range(count):
        first = pl.multiple_of(partner(here, shift, count) * height, height)
        outs[shift][...] = total[pl.ds(first, height), :].astype(BF16)


def project_out(x, weight):
    count = lax.axis_size("head")
    chunks, per_dest, depth = x.shape
    rows = chunks * per_dest
    width = weight.shape[1]
    return pl.pallas_call(
        output_kernel,
        out_shape=[jax.ShapeDtypeStruct((rows // count, width), BF16)] * count,
        in_specs=[VMEM, VMEM],
        out_specs=[VMEM] * count,
        scratch_shapes=[pltpu.VMEM((rows, depth), F32), pltpu.VMEM((rows, width), F32)],
        compiler_params=params(8 * MIB),
        cost_estimate=cost(2 * rows * weight.size, weight.size * 2),
        name="output",
    )(x, weight)


def body(
    token_ids,
    suffix_lengths,
    embedding,
    attn_gain,
    qkv_weight,
    out_weight,
    prefix_keys,
    prefix_values,
    suffix_keys,
    suffix_values,
):
    steps, batch = token_ids.shape
    rows = steps * batch
    n_ctx = lax.axis_size("ctx")
    n_head = lax.axis_size("head")
    heads, block_context, head_dim = prefix_keys.shape
    width = embedding.shape[1]
    columns = qkv_weight.shape[2]
    group = columns * n_ctx // head_dim - 2
    context = block_context * n_ctx
    capacity = 2 * rows // n_ctx
    qkv_weight = jnp.transpose(qkv_weight, (1, 2, 0))
    if embedding.shape[0] % 8 == 0 and capacity % 8 == 0:
        packed, places, crowded = lookup_packed(token_ids, embedding, capacity)

        def rest():
            found = lookup_rest(token_ids, places, embedding)
            return exchange(join_copies(exchange(found, "ctx")), "ctx")

        def nothing():
            return jnp.zeros((n_ctx, rows, width // n_ctx), BF16)

        features = lax.cond(crowded[0] > 0, rest, nothing)
        packed = exchange(spread(packed, features, 4 * qkv_weight.size), "ctx")
        packed = (packed, places)
    else:
        joined = join_copies(exchange(lookup_all(token_ids, embedding), "ctx"))
        features, packed = exchange(joined, "ctx"), ()
    *pieces, cosine, sine = project(
        features, attn_gain, qkv_weight, suffix_lengths, steps, context, head_dim, packed
    )
    pieces = send_pieces(pieces, "head")
    united = norm_copies(pieces, heads * columns, width * n_head)
    united = exchange(united, "ctx")
    packet, sums, maxima, totals = attend(
        united,
        columns,
        cosine,
        sine,
        prefix_keys,
        prefix_values,
        suffix_lengths,
        suffix_keys,
        suffix_values,
    )
    parts = exchange(packet, "ctx")
    attention = merge_copies(parts, sums, maxima, totals, group, rows // n_ctx)
    attention = exchange(attention, "ctx")
    pieces = send_pieces(project_out(attention, out_weight), "head")
    result = pieces[0].astype(F32)
    for piece in pieces[1:]:
        result = result + piece.astype(F32)
    return result.astype(BF16).reshape(batch // n_head, steps, -1)


def solution(mesh):
    placed = (
        P(),
        P(),
        P("ctx", "head"),
        P("head"),
        P("head", None, "ctx"),
        P("head", "ctx"),
        P("head", "ctx", None),
        P("head", "ctx", None),
        P("ctx", None, "head", None),
        P("ctx", None, "head", None),
    )
    return jax.shard_map(
        body, mesh=mesh, in_specs=placed, out_specs=P("head", None, "ctx"), check_vma=False
    )
```
